32 devices in a mesh: samples: 8 (over z, y), snps: 4 (over x, core).
Axes of the slice: x: 2, y: 2, z: 4, core: 2. Of those that a mesh axis runs over, the one named last changes fastest.
Arguments:
- genotype: int32 [4096, 1536], P('samples', 'snps'), may hold values from 0 to 2
- mask: int32 [4096, 1536], P('samples', 'snps'), may hold values 0 or 1
Outputs:
- blocks: float32 [4096, 2560], P('samples', 'snps')
The draws below stay inside these ranges and needn't reach their ends.
All inputs are finite; a program needn't handle non-finite values. No bound on the sum of `mask` on one device may be relied on, other than what follows from the above.
Results may differ from the reference program's by a relative error of at most 0.0014.
Values may be sent and summed in bfloat16 or wider, within the bound.
No kernel may reach another device: no remote copies, remote signals or barrier semaphores. Data moves between devices by JAX's collectives and lax.ppermute only.
A program may use at most 128 MiB of HBM per device.

```python
import jax
import jax.numpy as jnp
from jax import lax

SNPS = 1536
SAMPLE_DEV = 512
SAMPLES = 4096
OFFSETS = 5
N_SAMPLES = 8


def draw_genotype(key, part):
    base_key = jax.random.fold_in(key, 11)
    key_percent = jax.random.fold_in(base_key, 1)
    key_first = jax.random.fold_in(base_key, 2)
    key_second = jax.random.fold_in(base_key, 3)
    percent = jax.random.randint(key_percent, (1, SNPS), 5, 31)
    sample_rows = lax.broadcasted_iota(jnp.int32, (SAMPLES, 1), 0)
    limit = percent * (SAMPLES + 2 * sample_rows)
    first_allele = jax.random.randint(key_first, (SAMPLES, SNPS), 0, 100) * SAMPLES
    second_allele = jax.random.randint(key_second, (SAMPLES, SNPS), 0, 100) * SAMPLES
    return (first_allele < limit).astype(jnp.int32) + (second_allele < limit).astype(jnp.int32)


def place_ends(values, rng, smallest, top_value):
    dims = values.shape
    place = [jax.random.randint(jax.random.fold_in(rng, axis), (), 0, dims[axis]) for axis in range(len(dims))]
    values = values.at[tuple(place)].set(smallest)
    longest = dims.index(max(dims))
    place[longest] = (place[longest] + 1) % dims[longest]
    return values.at[tuple(place)].set(top_value)


def setup_inputs(seed: int = 0) -> dict:
    splits = jax.random.split(jax.random.key(seed), 3)
    genotype = draw_genotype(jax.random.fold_in(splits[2], 71), 0)
    mask = place_ends((jax.random.randint(splits[1], (SAMPLES, SNPS), 0, 10) < 9).astype(jnp.int32), jax.random.fold_in(splits[1], 1), 0, 1)
    return dict(genotype=genotype, mask=mask)


def standardize(genotype, mask):
    dosage = genotype.astype(jnp.float32)
    observed_mask = mask.astype(jnp.float32)
    allele_sum = lax.optimization_barrier(jnp.sum(dosage * observed_mask, axis=0))
    observed_sum = lax.optimization_barrier(jnp.sum(observed_mask, axis=0))
    frequency = (allele_sum + 1.0) / (2.0 * observed_sum + 2.0)
    scaled = observed_mask * (dosage - 2.0 * frequency) / jnp.sqrt(2.0 * frequency * (1.0 - frequency))
    return scaled.astype(jnp.bfloat16)

def reference(genotype, mask):
    standard = standardize(genotype, mask)

    def block_row(block_index):
        begin = (block_index * SAMPLE_DEV).astype(jnp.int32)
        own_rows = lax.dynamic_slice_in_dim(standard, begin, SAMPLE_DEV, 0)
        rolled = jnp.roll(standard, -begin, axis=0)[:OFFSETS * SAMPLE_DEV]
        product = lax.dot_general(own_rows, rolled, (((1,), (1,)), ((), ())), preferred_element_type=jnp.float32)
        return product / SNPS
    result = lax.map(block_row, jnp.arange(N_SAMPLES, dtype=jnp.int32))
    return result.reshape(SAMPLES, OFFSETS * SAMPLE_DEV)
```

```python
import jax
import jax.numpy as jnp
from jax import lax
from jax.sharding import PartitionSpec as P


def send(value, axis, route):
    count = lax.axis_size(axis)
    pairs = [(source, route(source)) for source in range(count)]
    return lax.ppermute(value, axis, [pair for pair in pairs if pair[1] is not None])


def swap_core(value):
    return send(value, "snps", lambda s: s ^ 1)


def add_over_samples(value):
    count = lax.axis_size("samples")
    if count & (count - 1):
        return lax.psum(value, "samples")
    step = 1
    while step < count:
        value = value + send(value, "samples", lambda s, step=step: s ^ step)
        step *= 2
    return value


def standardize(calls, allele_sum, observed_sum):
    frequency = (allele_sum + 1.0) / (2.0 * observed_sum + 2.0)
    shift = 1.0 + 2.0 * frequency
    scale = 1.0 / jnp.sqrt(2.0 * frequency * (1.0 - frequency))
    wide = calls.astype(jnp.float32)
    return jnp.where(wide > 0.0, (wide - shift) * scale, 0.0).astype(jnp.bfloat16)


def product(own_rows, other_rows):
    return lax.dot_general(
        own_rows, other_rows, (((1,), (1,)), ((), ())), preferred_element_type=jnp.float32
    )


def per_device(genotype, mask):
    samples = lax.axis_size("samples")
    parts = lax.axis_size("snps")
    assert samples % 4 == 0 and parts == 4
    rows = genotype.shape[0]
    snp_total = genotype.shape[1] * parts
    offsets = samples // 2 + 1
    width = rows * offsets // parts
    turns = samples // 4

    calls = (mask * (genotype + 1)).astype(jnp.bfloat16)
    sums = jnp.stack([
        jnp.sum((genotype * mask).astype(jnp.float32), axis=0),
        jnp.sum(mask.astype(jnp.float32), axis=0),
    ])

    along = lambda s: (s - 2) % samples
    even = lax.axis_index("samples") % 2 == 0
    line = [calls]
    for _ in range(turns):
        line.append(send(line[-1], "samples", along))
    side = [send(calls, "samples", lambda s: s - 1 if s % 2 else None)]
    for t in range(1, turns):
        side.append(send(line[t], "samples", lambda s: s ^ 1))
    side.append(send(line[turns], "samples", lambda s: None if s % 2 else s + 1))

    blocks = [calls]
    for k in range(1, offsets):
        if k % 2 == 0:
            blocks.append(line[k // 2])
        else:
            blocks.append(jnp.where(even, side[k // 2], side[k // 2 + 1]))
    partner = [swap_core(block) for block in blocks]

    sums = add_over_samples(sums)
    partner_sums = swap_core(sums)

    own = [standardize(block, sums[0], sums[1]) for block in blocks]
    other = [standardize(block, partner_sums[0], partner_sums[1]) for block in partner]
    every = jnp.concatenate(
        [jnp.concatenate(own, axis=0), jnp.concatenate(other, axis=0)], axis=1
    )
    mine = lax.axis_index("snps")
    left = every[:rows]

    def strip(index):
        begin = (index * width).astype(jnp.int32)
        return product(left, lax.dynamic_slice_in_dim(every, begin, width, 0))

    theirs = strip(mine ^ 2).astype(jnp.bfloat16)
    received = send(theirs, "snps", lambda s: s ^ 2)
    return (strip(mine) + received.astype(jnp.float32)) / snp_total


def solution(mesh):
    return jax.shard_map(
        per_device,
        mesh=mesh,
        in_specs=(P("samples", "snps"), P("samples", "snps")),
        out_specs=P("samples", "snps"),
        check_vma=False,
    )
```

```python
import functools
import math

import jax
import jax.numpy as jnp
from jax import lax
from jax.experimental import pallas as pl
from jax.experimental.pallas import tpu as pltpu
from jax.sharding import PartitionSpec as P


def send(value, axis, route):
    count = lax.axis_size(axis)
    pairs = [(source, route(source)) for source in range(count)]
    return lax.ppermute(value, axis, [pair for pair in pairs if pair[1] is not None])


def swap_core(value):
    return send(value, "snps", lambda s: s ^ 1)


def arrival(piece):
    k, half = piece
    return k + 0.5 * half + (1.6 if k % 2 else 0.0)


def strips(samples):
    whole_count = (samples + 2) // 4
    result = []
    for strip in range(4):
        first = strip * (samples + 2) // 4
        begin = first + strip % 2
        wholes = [divmod(begin + n, 2) for n in range(whole_count)]
        cut = divmod(first if strip % 2 else first + whole_count, 2)
        result.append((sorted(wholes, key=arrival), wholes, cut))
    return result


def call_kernel(body, shapes, operands, specs, flops, moved, **more):
    return pl.pallas_call(
        body,
        out_shape=shapes,
        in_specs=specs,
        compiler_params=pltpu.CompilerParams(vmem_limit_bytes=24 * 2**20),
        cost_estimate=pl.CostEstimate(flops=flops, bytes_accessed=moved, transcendentals=0),
        **more,
    )(*operands)


VMEM = pl.BlockSpec(memory_space=pltpu.VMEM)
SMEM = pl.BlockSpec(memory_space=pltpu.SMEM)
ANY = pl.BlockSpec(memory_space=pl.ANY)


def encode_body(genotype_ref, mask_ref, whole_ref, first_ref, second_ref, sums_ref):
    half = pl.program_id(0)
    mask = mask_ref[...]
    dosage = mask * genotype_ref[...]
    calls = (dosage + mask).astype(jnp.float32).astype(jnp.bfloat16)
    whole_ref[...] = calls

    @pl.when(half == 0)
    def _():
        first_ref[...] = calls
        sums_ref[...] = jnp.zeros_like(sums_ref)

    @pl.when(half == 1)
    def _():
        second_ref[...] = calls

    sums_ref[0:1, :] += jnp.sum(dosage.astype(jnp.float32), axis=0, keepdims=True)
    sums_ref[1:2, :] += jnp.sum(mask.astype(jnp.float32), axis=0, keepdims=True)


def encode(genotype, mask):
    rows, columns = genotype.shape
    half = rows // 2
    calls = lambda n: jax.ShapeDtypeStruct((n, columns), jnp.bfloat16)
    block = pl.BlockSpec((half, columns), lambda i: (i, 0))
    fixed = lambda n: pl.BlockSpec((n, columns), lambda i: (0, 0))
    return pl.pallas_call(
        encode_body,
        name="encode",
        grid=(2,),
        out_shape=(calls(rows), calls(half), calls(half), jax.ShapeDtypeStruct((2, columns), jnp.float32)),
        in_specs=[block, block],
        out_specs=(block, fixed(half), fixed(half), fixed(2)),
        compiler_params=pltpu.CompilerParams(vmem_limit_bytes=16 * 2**20),
    )(genotype, mask)


def factors(sums):
    frequency = (sums[0:1] + 1.0) / (2.0 * sums[1:2] + 2.0)
    return 1.0 + 2.0 * frequency, 1.0 / jnp.sqrt(2.0 * frequency * (1.0 - frequency))


def standardized(calls, shift, scale):
    wide = calls.astype(jnp.float32)
    return jnp.where(wide > 0.0, (wide - shift) * scale, 0.0).astype(jnp.bfloat16)


def left_body(calls_ref, other_ref, sums_ref, other_sums_ref, left_ref, shift_ref, scale_ref):
    part = calls_ref.shape[1]
    for n, (rows_ref, counts_ref) in enumerate(((calls_ref, sums_ref), (other_ref, other_sums_ref))):
        shift, scale = factors(counts_ref[...])
        shift_ref[:, pl.ds(n * part, part)] = shift
        scale_ref[:, pl.ds(n * part, part)] = scale
        left_ref[:, pl.ds(n * part, part)] = standardized(rows_ref[...], shift, scale)


def fill_right(choice, parity, cases, refs, shift_ref, scale_ref, right_ref):
    part = refs[0].shape[1]
    for strip, by_parity in enumerate(cases):
        for odd, (at, begin) in enumerate(by_parity):
            same = by_parity[0] == by_parity[1]
            if odd and same:
                continue
            wanted = choice == strip if same else (choice == strip) & (parity == odd)

            @pl.when(wanted)
            def _(at=at, begin=begin):
                for n in range(2):
                    columns = pl.ds(n * part, part)
                    right_ref[:, columns] = standardized(
                        refs[at + n][pl.ds(begin, right_ref.shape[0]), :],
                        shift_ref[:, columns], scale_ref[:, columns],
                    )


def multiply(left, right):
    return lax.dot_general(
        left, right, (((1,), (1,)), ((), ())), preferred_element_type=jnp.float32
    )


def theirs_body(cases, down, where_ref, left_ref, shift_ref, scale_ref, *rest):
    *refs, out_ref, right_ref = rest
    fill_right(where_ref[0], where_ref[1], cases, refs, shift_ref, scale_ref, right_ref)
    out_ref[...] = multiply(left_ref[...], right_ref[...]) * down


def ours_body(cases, places, up, first, where_ref, left_ref, shift_ref, scale_ref, got_ref, *rest):
    *refs, out_ref, right_ref, total_ref, sem = rest
    if not first:
        refs = refs[:-1]
    fill_right(where_ref[0], where_ref[1], cases, refs, shift_ref, scale_ref, right_ref)
    ours = multiply(left_ref[...], right_ref[...])
    total_ref[...] = ours * up[0] + got_ref[...] * up[1]
    width = total_ref.shape[1]
    for strip, begin in enumerate(places):

        @pl.when(where_ref[0] == strip)
        def _(begin=begin):
            copy = pltpu.make_async_copy(total_ref, out_ref.at[:, pl.ds(begin, width)], sem)
            copy.start()
            copy.wait()


def per_device(genotype, mask):
    samples = lax.axis_size("samples")
    parts = lax.axis_size("snps")
    assert samples % 4 == 0 and samples & (samples - 1) == 0 and parts == 4
    rows, snp_part = genotype.shape
    snp_total = snp_part * parts
    turns = samples // 4
    half_rows = rows // 2
    width = rows * (samples // 2 + 1) // parts

    calls, first, second, sums = encode(genotype, mask)

    along = lambda s: (s - 2) % samples
    line = [[first, second]]
    for _ in range(1, turns + 1):
        line.append([send(line[-1][h], "samples", along) for h in range(2)])
    beside = send(calls, "samples", lambda s: s - 1 if s % 2 else None)
    side = [None]
    for t in range(1, turns):
        side.append([send(line[t][h], "samples", lambda s: s ^ 1) for h in range(2)])
    side.append([send(line[turns][h], "samples", lambda s: None if s % 2 else s + 1) for h in range(2)])

    for bit in range(samples.bit_length() - 1):
        sums = sums + send(sums, "samples", lambda s, step=1 << bit: s ^ step)
    other_sums = swap_core(sums)

    both = {("own", None): (calls, swap_core(calls)), ("y", 0): (beside, swap_core(beside))}
    for t in range(1, turns + 1):
        for h in range(2):
            both["z", t, h] = (line[t][h], swap_core(line[t][h]))
            both["y", t, h] = (side[t][h], swap_core(side[t][h]))

    def source(k, h, odd):
        if k == 0:
            return ("own", None), h * half_rows
        if k % 2 == 0:
            return ("z", k // 2, h), 0
        if k == 1 and not odd:
            return ("y", 0), h * half_rows
        return ("y", (k + odd) // 2, h), 0

    part = snp_part
    line_shape = jax.ShapeDtypeStruct((1, 2 * part), jnp.float32)
    left, shift, scale = call_kernel(
        left_body,
        (jax.ShapeDtypeStruct((rows, 2 * part), jnp.bfloat16), line_shape, line_shape),
        (*both["own", None], sums, other_sums), [VMEM] * 4, 10 * rows * part, 4 * rows * part,
        out_specs=(VMEM, VMEM, VMEM),
    )

    device = lax.axis_index("snps").astype(jnp.int32)
    parity = (lax.axis_index("samples") % 2).astype(jnp.int32)
    table = strips(samples)
    bound = snp_total / 2 * 4 * (samples * rows + 1) / 3
    down = 2.0 ** -math.ceil(math.log2(bound / 32768.0))
    count = len(table[0][0])
    quarter = half_rows // 2

    def gather(n):
        keys, cases, places = [], [], []
        for strip, (by_arrival, natural, cut) in enumerate(table):
            piece = by_arrival[n] if n < count else cut
            by_parity = []
            for odd in range(2):
                key, begin = source(*piece, odd)
                if key not in keys:
                    keys.append(key)
                if n == count and strip % 2:
                    begin += quarter
                by_parity.append((2 * keys.index(key), begin))
            cases.append(tuple(by_parity))
            if n < count:
                places.append(natural.index(piece) * half_rows + (strip % 2) * quarter)
            else:
                places.append(0 if strip % 2 else count * half_rows)
        return [array for key in keys for array in both[key]], tuple(cases), tuple(places)

    out = None
    pieces = []
    for n in range(count + 1):
        arrays, cases, places = gather(n)
        columns = half_rows if n < count else quarter
        flops = 2 * rows * 2 * part * columns
        right = pltpu.VMEM((columns, 2 * part), jnp.bfloat16)
        theirs = call_kernel(
            functools.partial(theirs_body, cases, down),
            jax.ShapeDtypeStruct((rows, columns), jnp.float32),
            (jnp.stack([device ^ 2, parity]), left, shift, scale, *arrays),
            [SMEM] + [VMEM] * (3 + len(arrays)), flops, 2 * rows * columns,
            out_specs=VMEM, scratch_shapes=[right],
        )
        got = send(theirs.astype(jnp.float16), "snps", lambda s: s ^ 2)
        pieces.append((arrays, cases, places, columns, flops, right, got))
    for n, (arrays, cases, places, columns, flops, right, got) in enumerate(pieces):
        last = () if out is None else (out,)
        operands = (jnp.stack([device, parity]), left, shift, scale, got.astype(jnp.float32), *arrays, *last)
        out = call_kernel(
            functools.partial(ours_body, cases, places, (1.0 / snp_total, 1.0 / (down * snp_total)), n == 0),
            jax.ShapeDtypeStruct((rows, width), jnp.float32), operands,
            [SMEM] + [VMEM] * (4 + len(arrays)) + [ANY] * len(last), flops, 4 * rows * columns,
            out_specs=ANY,
            scratch_shapes=[right, pltpu.VMEM((rows, columns), jnp.float32), pltpu.SemaphoreType.DMA],
            input_output_aliases={len(operands) - 1: 0} if last else {},
        )
    return out


def solution(mesh):
    return jax.shard_map(
        per_device,
        mesh=mesh,
        in_specs=(P("samples", "snps"), P("samples", "snps")),
        out_specs=P("samples", "snps"),
        check_vma=False,
    )
```

```python
import functools
import math

import jax
import jax.numpy as jnp
from jax import lax
from jax.experimental import pallas as pl
from jax.experimental.pallas import tpu as pltpu
from jax.sharding import PartitionSpec as P


def send(value, axis, route):
    count = lax.axis_size(axis)
    pairs = [(source, route(source)) for source in range(count)]
    return lax.ppermute(value, axis, [pair for pair in pairs if pair[1] is not None])


def swap_core(value):
    return send(value, "snps", lambda s: s ^ 1)


def arrival(piece):
    k, half = piece
    return k + 0.5 * half + (1.6 if k % 2 else 0.0)


def strips(samples):
    whole_count = (samples + 2) // 4
    result = []
    for strip in range(4):
        first = strip * (samples + 2) // 4
        begin = first + strip % 2
        wholes = [divmod(begin + n, 2) for n in range(whole_count)]
        cut = divmod(first if strip % 2 else first + whole_count, 2)
        result.append((sorted(wholes, key=arrival), wholes, cut))
    return result


def call_kernel(body, shapes, operands, specs, flops, moved, **more):
    return pl.pallas_call(
        body,
        out_shape=shapes,
        in_specs=specs,
        compiler_params=pltpu.CompilerParams(vmem_limit_bytes=24 * 2**20),
        cost_estimate=pl.CostEstimate(flops=flops, bytes_accessed=moved, transcendentals=0),
        **more,
    )(*operands)


VMEM = pl.BlockSpec(memory_space=pltpu.VMEM)
SMEM = pl.BlockSpec(memory_space=pltpu.SMEM)
ANY = pl.BlockSpec(memory_space=pl.ANY)


def encode_body(genotype_ref, mask_ref, whole_ref, first_ref, second_ref, sums_ref,
                dosage_in, mask_in, sems):
    rows = first_ref.shape[0]
    copies = []
    for half in range(2):
        at = pl.ds(half * rows, rows)
        copies.append([
            pltpu.make_async_copy(source.at[at], target.at[at], sems.at[2 * half + n])
            for n, (source, target) in enumerate(((genotype_ref, dosage_in), (mask_ref, mask_in)))
        ])
    for copy in copies[0] + copies[1]:
        copy.start()
    totals = []
    for half, part_ref in enumerate((first_ref, second_ref)):
        for copy in copies[half]:
            copy.wait()
        at = pl.ds(half * rows, rows)
        mask = mask_in[at, :]
        dosage = mask * dosage_in[at, :]
        calls = (dosage + mask).astype(jnp.float32).astype(jnp.bfloat16)
        whole_ref[at, :] = calls
        part_ref[...] = calls
        totals.append([
            jnp.sum(value.astype(jnp.float32), axis=0, keepdims=True) for value in (dosage, mask)
        ])
    for n in range(2):
        sums_ref[n : n + 1, :] = totals[0][n] + totals[1][n]


def encode(genotype, mask):
    rows, columns = genotype.shape
    half = rows // 2
    calls = lambda n: jax.ShapeDtypeStruct((n, columns), jnp.bfloat16)
    return pl.pallas_call(
        encode_body,
        name="encode",
        out_shape=(calls(rows), calls(half), calls(half), jax.ShapeDtypeStruct((2, columns), jnp.float32)),
        in_specs=[ANY, ANY],
        out_specs=(VMEM,) * 4,
        scratch_shapes=[
            pltpu.VMEM((rows, columns), jnp.int32),
            pltpu.VMEM((rows, columns), jnp.int32),
            pltpu.SemaphoreType.DMA((4,)),
        ],
        compiler_params=pltpu.CompilerParams(vmem_limit_bytes=40 * 2**20),
    )(pltpu.with_memory_space_constraint(genotype, pltpu.HBM), pltpu.with_memory_space_constraint(mask, pltpu.HBM))


def factors(sums):
    frequency = (sums[0:1] + 1.0) / (2.0 * sums[1:2] + 2.0)
    return 1.0 + 2.0 * frequency, 1.0 / jnp.sqrt(2.0 * frequency * (1.0 - frequency))


def standardized(calls, shift, scale):
    wide = calls.astype(jnp.float32)
    return jnp.where(wide > 0.0, (wide - shift) * scale, 0.0).astype(jnp.bfloat16)


def left_body(calls_ref, sums_ref, left_ref):
    left_ref[...] = standardized(calls_ref[...], *factors(sums_ref[...]))


def multiply(left, right):
    return lax.dot_general(
        left, right, (((1,), (1,)), ((), ())), preferred_element_type=jnp.float32
    )


def products_body(cases, where_ref, left_ref, sums_ref, *rest):
    *refs, keep_ref, away_ref, right_ref = rest
    shift, scale = factors(sums_ref[...])
    for strip, by_parity in cases:
        for odd, (at, begin) in enumerate(by_parity):

            def fill(at=at, begin=begin):
                rows = refs[at][pl.ds(begin, right_ref.shape[0]), :]
                right_ref[...] = standardized(rows, shift, scale)

            if by_parity[0] != by_parity[1]:
                pl.when(where_ref[1] == odd)(fill)
            elif not odd:
                fill()
        place = where_ref[0] ^ strip
        for bit, target_ref in enumerate((keep_ref, away_ref)):

            @pl.when(place % 2 == bit)
            def _(target_ref=target_ref, place=place):
                target_ref[place // 2] = multiply(left_ref[...], right_ref[...])


def products_more_body(cases, where_ref, left_ref, sums_ref, *rest):
    *refs, _, _, keep_ref, away_ref, right_ref = rest
    products_body(cases, where_ref, left_ref, sums_ref, *refs, keep_ref, away_ref, right_ref)


def add_body(places, up, where_ref, keep_ref, other_ref, got_ref, *rest):
    out_ref, total_ref, sem = rest[-3:]
    total_ref[...] = (keep_ref[0] + other_ref[0]) * up[0] + got_ref[...] * up[1]
    width = total_ref.shape[1]
    for strip, begin in enumerate(places):

        @pl.when(where_ref[0] == strip)
        def _(begin=begin):
            copy = pltpu.make_async_copy(total_ref, out_ref.at[:, pl.ds(begin, width)], sem)
            copy.start()
            copy.wait()


def per_device(genotype, mask):
    samples = lax.axis_size("samples")
    parts = lax.axis_size("snps")
    assert samples % 4 == 0 and samples & (samples - 1) == 0 and parts == 4
    rows, snp_part = genotype.shape
    snp_total = snp_part * parts
    turns = samples // 4
    half_rows = rows // 2
    width = rows * (samples // 2 + 1) // parts

    calls, first, second, sums = encode(genotype, mask)

    along = lambda s: (s - 2) % samples
    line = [[first, second]]
    for _ in range(1, turns + 1):
        line.append([send(line[-1][h], "samples", along) for h in range(2)])
    beside = send(calls, "samples", lambda s: s - 1 if s % 2 else None)
    side = [None]
    for t in range(1, turns):
        side.append([send(line[t][h], "samples", lambda s: s ^ 1) for h in range(2)])
    side.append([
        send(line[turns][h], "samples", lambda s: None if s % 2 else s + 1)
        for h in range(2)
    ])

    for bit in range(samples.bit_length() - 1):
        sums = sums + send(sums, "samples", lambda s, step=1 << bit: s ^ step)

    def source(k, h, odd):
        if k == 0:
            return calls, h * half_rows
        if k % 2 == 0:
            return line[k // 2][h], 0
        if k == 1 and not odd:
            return beside, h * half_rows
        return side[(k + odd) // 2][h], 0

    left = call_kernel(
        left_body, jax.ShapeDtypeStruct((rows, snp_part), jnp.bfloat16), (calls, sums),
        [VMEM] * 2, 5 * rows * snp_part, 4 * rows * snp_part, out_specs=VMEM,
    )
    device = lax.axis_index("snps").astype(jnp.int32)
    parity = (lax.axis_index("samples") % 2).astype(jnp.int32)
    where = jnp.stack([device, parity])
    table = strips(samples)
    bound = snp_total / 2 * 4 * (samples * rows + 1) / 3
    down = 2.0 ** -math.ceil(math.log2(bound / 32768.0))
    count = len(table[0][0])
    quarter = half_rows // 2

    def products(n, chosen, so_far):
        columns = half_rows if n < count else quarter
        arrays, cases = [], []
        for strip in chosen:
            by_arrival, _, cut = table[strip]
            by_parity = []
            for odd in range(2):
                array, begin = source(*(by_arrival[n] if n < count else cut), odd)
                at = next((i for i, known in enumerate(arrays) if known is array), len(arrays))
                if at == len(arrays):
                    arrays.append(array)
                if n == count and strip % 2:
                    begin += quarter
                by_parity.append((at, begin))
            cases.append((strip, tuple(by_parity)))
        shape = jax.ShapeDtypeStruct((2, rows, columns), jnp.float32)
        operands = (where, left, sums, *arrays, *so_far)
        return call_kernel(
            functools.partial(products_body if not so_far else products_more_body, tuple(cases)),
            (shape, shape), operands, [SMEM] + [VMEM] * (len(operands) - 1),
            2 * rows * snp_part * columns * len(chosen), 4 * rows * columns,
            out_specs=(VMEM, VMEM),
            scratch_shapes=[pltpu.VMEM((columns, snp_part), jnp.bfloat16)],
            input_output_aliases={len(operands) - 2 + i: i for i in range(len(so_far))},
        )

    pieces = []
    for n in range(count + 1):
        late = [
            strip for strip, (by_arrival, _, cut) in enumerate(table)
            if (by_arrival[n] if n < count else cut)[0] >= 2 * turns - 1
        ]
        both = ()
        for chosen in ([s for s in range(4) if s not in late], late):
            if chosen:
                both = products(n, chosen, both)
        keep, away = both
        other = swap_core(away)
        theirs = ((keep[1] + other[1]) * down).astype(jnp.float16)
        got = send(theirs, "snps", lambda s: s ^ 2).astype(jnp.float32)
        pieces.append((keep, other, got))
    out = None
    for n, operands in enumerate(pieces):
        places = []
        for strip, (by_arrival, natural, _) in enumerate(table):
            if n < count:
                places.append(natural.index(by_arrival[n]) * half_rows + (strip % 2) * quarter)
            else:
                places.append(0 if strip % 2 else count * half_rows)
        columns = operands[2].shape[1]
        last = () if out is None else (out,)
        operands = (where, *operands, *last)
        out = call_kernel(
            functools.partial(add_body, tuple(places), (1.0 / snp_total, 1.0 / (down * snp_total))),
            jax.ShapeDtypeStruct((rows, width), jnp.float32), operands,
            [SMEM] + [VMEM] * 3 + [ANY] * len(last), rows * columns, 4 * rows * columns,
            out_specs=ANY,
            scratch_shapes=[pltpu.VMEM((rows, columns), jnp.float32), pltpu.SemaphoreType.DMA],
            input_output_aliases={len(operands) - 1: 0} if last else {},
        )
    return out


def solution(mesh):
    return jax.shard_map(
        per_device,
        mesh=mesh,
        in_specs=(P("samples", "snps"), P("samples", "snps")),
        out_specs=P("samples", "snps"),
        check_vma=False,
    )
```

```python
import functools
import math

import jax
import jax.numpy as jnp
from jax import lax
from jax.experimental import pallas as pl
from jax.experimental.pallas import tpu as pltpu
from jax.sharding import PartitionSpec as P


def send(value, axis, route):
    count = lax.axis_size(axis)
    pairs = [(source, route(source)) for source in range(count)]
    return lax.ppermute(value, axis, [pair for pair in pairs if pair[1] is not None])


def swap_core(value):
    return send(value, "snps", lambda s: s ^ 1)


def arrival(piece):
    k, half = piece
    return k + 0.5 * half + (1.6 if k % 2 else 0.0)


def strips(samples):
    whole_count = (samples + 2) // 4
    result = []
    for strip in range(4):
        first = strip * (samples + 2) // 4
        begin = first + strip % 2
        wholes = [divmod(begin + n, 2) for n in range(whole_count)]
        cut = divmod(first if strip % 2 else first + whole_count, 2)
        result.append((sorted(wholes, key=arrival), wholes, cut))
    return result


def call_kernel(body, shapes, operands, specs, flops, moved, **more):
    return pl.pallas_call(
        body,
        out_shape=shapes,
        in_specs=specs,
        compiler_params=pltpu.CompilerParams(vmem_limit_bytes=24 * 2**20),
        cost_estimate=pl.CostEstimate(flops=flops, bytes_accessed=moved, transcendentals=0),
        **more,
    )(*operands)


VMEM = pl.BlockSpec(memory_space=pltpu.VMEM)
ANY = pl.BlockSpec(memory_space=pl.ANY)


def encode_body(genotype_ref, mask_ref, whole_ref, first_ref, second_ref, sums_ref,
                dosage_in, mask_in, sems):
    rows = first_ref.shape[0]
    copies = []
    for half in range(2):
        at = pl.ds(half * rows, rows)
        copies.append([
            pltpu.make_async_copy(source.at[at], target.at[at], sems.at[2 * half + n])
            for n, (source, target) in enumerate(((genotype_ref, dosage_in), (mask_ref, mask_in)))
        ])
    for copy in copies[0] + copies[1]:
        copy.start()
    totals = []
    for half, part_ref in enumerate((first_ref, second_ref)):
        for copy in copies[half]:
            copy.wait()
        at = pl.ds(half * rows, rows)
        mask = mask_in[at, :]
        dosage = mask * dosage_in[at, :]
        calls = (dosage + mask).astype(jnp.float32).astype(jnp.bfloat16)
        whole_ref[at, :] = calls
        part_ref[...] = calls
        totals.append([
            jnp.sum(value.astype(jnp.float32), axis=0, keepdims=True) for value in (dosage, mask)
        ])
    for n in range(2):
        sums_ref[n : n + 1, :] = totals[0][n] + totals[1][n]


def encode(genotype, mask):
    rows, columns = genotype.shape
    half = rows // 2
    calls = lambda n: jax.ShapeDtypeStruct((n, columns), jnp.bfloat16)
    return pl.pallas_call(
        encode_body,
        name="encode",
        out_shape=(calls(rows), calls(half), calls(half), jax.ShapeDtypeStruct((2, columns), jnp.float32)),
        in_specs=[ANY, ANY],
        out_specs=(VMEM,) * 4,
        scratch_shapes=[
            pltpu.VMEM((rows, columns), jnp.int32),
            pltpu.VMEM((rows, columns), jnp.int32),
            pltpu.SemaphoreType.DMA((4,)),
        ],
        compiler_params=pltpu.CompilerParams(vmem_limit_bytes=40 * 2**20),
    )(pltpu.with_memory_space_constraint(genotype, pltpu.HBM), pltpu.with_memory_space_constraint(mask, pltpu.HBM))


def factors(sums):
    frequency = (sums[0:1] + 1.0) / (2.0 * sums[1:2] + 2.0)
    return 1.0 + 2.0 * frequency, 1.0 / jnp.sqrt(2.0 * frequency * (1.0 - frequency))


def standardized(calls, shift, scale):
    wide = calls.astype(jnp.float32)
    return jnp.where(wide > 0.0, (wide - shift) * scale, 0.0).astype(jnp.bfloat16)


def left_body(calls_ref, sums_ref, more_ref, left_ref, factors_ref):
    shift, scale = factors(sums_ref[...] + more_ref[...])
    factors_ref[0:1, :] = shift
    factors_ref[1:2, :] = scale
    left_ref[...] = standardized(calls_ref[...], shift, scale)


def multiply(left, right):
    return lax.dot_general(
        left, right, (((1,), (1,)), ((), ())), preferred_element_type=jnp.float32
    )


def products_body(cases, down, left_ref, factors_ref, *rest):
    *refs, keep_ref, away_ref, right_ref = rest
    shift, scale = factors_ref[0:1, :], factors_ref[1:2, :]
    device = lax.axis_index("snps")
    parity = lax.axis_index("samples") % 2
    for strip, by_parity in cases:
        for odd, (at, begin) in enumerate(by_parity):

            def fill(at=at, begin=begin):
                rows = refs[at][pl.ds(begin, right_ref.shape[0]), :]
                right_ref[...] = standardized(rows, shift, scale)

            if by_parity[0] != by_parity[1]:
                pl.when(parity == odd)(fill)
            elif not odd:
                fill()
        place = device ^ strip
        for bit, target_ref in enumerate((keep_ref, away_ref)):

            @pl.when(place % 2 == bit)
            def _(target_ref=target_ref, place=place):
                target_ref[place // 2] = multiply(left_ref[...], right_ref[...]) * down


def products_more_body(cases, down, left_ref, factors_ref, *rest):
    *refs, _, _, keep_ref, away_ref, right_ref = rest
    products_body(cases, down, left_ref, factors_ref, *refs, keep_ref, away_ref, right_ref)


def add_body(places, up, ours_ref, got_ref, *rest):
    out_ref, total_ref, sem = rest[-3:]
    total_ref[...] = (ours_ref[...] + got_ref[...]) * up
    device = lax.axis_index("snps")
    width = total_ref.shape[1]
    for strip, begin in enumerate(places):

        @pl.when(device == strip)
        def _(begin=begin):
            copy = pltpu.make_async_copy(total_ref, out_ref.at[:, pl.ds(begin, width)], sem)
            copy.start()
            copy.wait()


def per_device(genotype, mask):
    samples = lax.axis_size("samples")
    parts = lax.axis_size("snps")
    assert samples % 4 == 0 and samples & (samples - 1) == 0 and parts == 4
    rows, snp_part = genotype.shape
    snp_total = snp_part * parts
    turns = samples // 4
    half_rows = rows // 2
    width = rows * (samples // 2 + 1) // parts

    calls, first, second, sums = encode(genotype, mask)

    along = lambda s: (s - 2) % samples
    line = [[first, second]]
    for _ in range(1, turns + 1):
        line.append([send(line[-1][h], "samples", along) for h in range(2)])
    beside = send(calls, "samples", lambda s: s - 1 if s % 2 else None)
    side = [None] + [[send(line[t][h], "samples", lambda s: s ^ 1) for h in range(2)] for t in range(1, turns + 1)]

    for bit in range(samples.bit_length() - 1):
        more = send(sums, "samples", lambda s, step=1 << bit: s ^ step)
        if 2 << bit < samples:
            sums = sums + more

    def source(k, h, odd):
        if k == 0:
            return calls, h * half_rows
        if k % 2 == 0:
            return line[k // 2][h], 0
        if k == 1 and not odd:
            return beside, h * half_rows
        return side[(k + odd) // 2][h], 0

    left, pair = call_kernel(
        left_body,
        (jax.ShapeDtypeStruct((rows, snp_part), jnp.bfloat16), jax.ShapeDtypeStruct((2, snp_part), jnp.float32)),
        (calls, sums, more), [VMEM] * 3, 5 * rows * snp_part, 4 * rows * snp_part, out_specs=(VMEM, VMEM),
    )
    table = strips(samples)
    bound = snp_total / 2 * 4 * (samples * rows + 1) / 3
    down = 2.0 ** -math.ceil(math.log2(bound / 32768.0))
    count = len(table[0][0])
    quarter = half_rows // 2

    def products(n, chosen, so_far):
        columns = half_rows if n < count else quarter
        arrays, cases = [], []
        for strip in chosen:
            by_arrival, _, cut = table[strip]
            by_parity = []
            for odd in range(2):
                array, begin = source(*(by_arrival[n] if n < count else cut), odd)
                at = next((i for i, known in enumerate(arrays) if known is array), len(arrays))
                if at == len(arrays):
                    arrays.append(array)
                if n == count and strip % 2:
                    begin += quarter
                by_parity.append((at, begin))
            cases.append((strip, tuple(by_parity)))
        shape = jax.ShapeDtypeStruct((2, rows, columns), jnp.float32)
        operands = (left, pair, *arrays, *so_far)
        return call_kernel(
            functools.partial(products_body if not so_far else products_more_body, tuple(cases), down),
            (shape, shape), operands, [VMEM] * len(operands),
            2 * rows * snp_part * columns * len(chosen), 4 * rows * columns,
            out_specs=(VMEM, VMEM),
            scratch_shapes=[pltpu.VMEM((columns, snp_part), jnp.bfloat16)],
            input_output_aliases={len(operands) - 2 + i: i for i in range(len(so_far))},
        )

    pieces = []
    for n in range(count + 1):
        late = [
            strip for strip, (by_arrival, _, cut) in enumerate(table)
            if (by_arrival[n] if n < count else cut)[0] >= 2 * turns - 1
        ]
        both = ()
        for chosen in ([s for s in range(4) if s not in late], late):
            if chosen:
                both = products(n, chosen, both)
        keep, away = both
        summed = keep + swap_core(away.astype(jnp.float16)).astype(jnp.float32)
        got = send(summed[1].astype(jnp.float16), "snps", lambda s: s ^ 2)
        pieces.append((summed[0], got.astype(jnp.float32)))
    out = None
    for n, operands in enumerate(pieces):
        places = []
        for strip, (by_arrival, natural, _) in enumerate(table):
            if n < count:
                places.append(natural.index(by_arrival[n]) * half_rows + (strip % 2) * quarter)
            else:
                places.append(0 if strip % 2 else count * half_rows)
        columns = operands[1].shape[1]
        last = () if out is None else (out,)
        operands = (*operands, *last)
        out = call_kernel(
            functools.partial(add_body, tuple(places), 1.0 / (down * snp_total)),
            jax.ShapeDtypeStruct((rows, width), jnp.float32), operands,
            [VMEM] * 2 + [ANY] * len(last), rows * columns, 4 * rows * columns,
            out_specs=ANY,
            scratch_shapes=[pltpu.VMEM((rows, columns), jnp.float32), pltpu.SemaphoreType.DMA],
            input_output_aliases={len(operands) - 1: 0} if last else {},
        )
    return out


def solution(mesh):
    return jax.shard_map(
        per_device,
        mesh=mesh,
        in_specs=(P("samples", "snps"), P("samples", "snps")),
        out_specs=P("samples", "snps"),
        check_vma=False,
    )
```

```python
import functools
import math

import jax
import jax.numpy as jnp
from jax import lax
from jax.experimental import pallas as pl
from jax.experimental.pallas import tpu as pltpu
from jax.sharding import PartitionSpec as P


def send(value, axis, route):
    count = lax.axis_size(axis)
    pairs = [(source, route(source)) for source in range(count)]
    return lax.ppermute(value, axis, [pair for pair in pairs if pair[1] is not None])


def swap_core(value):
    return send(value, "snps", lambda s: s ^ 1)


def arrival(piece):
    k, half = piece
    return k + 0.5 * half + (1.6 if k % 2 else 0.0)


def strips(samples):
    whole_count = (samples + 2) // 4
    result = []
    for strip in range(4):
        first = strip * (samples + 2) // 4
        begin = first + strip % 2
        wholes = [divmod(begin + n, 2) for n in range(whole_count)]
        cut = divmod(first if strip % 2 else first + whole_count, 2)
        result.append((sorted(wholes, key=arrival), wholes, cut))
    return result


def call_kernel(body, shapes, operands, specs, flops, moved, **more):
    return pl.pallas_call(
        body,
        out_shape=shapes,
        in_specs=specs,
        compiler_params=pltpu.CompilerParams(vmem_limit_bytes=24 * 2**20),
        cost_estimate=pl.CostEstimate(flops=flops, bytes_accessed=moved, transcendentals=0),
        **more,
    )(*operands)


VMEM = pl.BlockSpec(memory_space=pltpu.VMEM)
ANY = pl.BlockSpec(memory_space=pl.ANY)


def encode_body(genotype_ref, mask_ref, whole_ref, first_ref, second_ref, sums_ref,
                dosage_in, mask_in, sems):
    rows = first_ref.shape[0]
    copies = []
    for half in range(2):
        at = pl.ds(half * rows, rows)
        copies.append([
            pltpu.make_async_copy(source.at[at], target.at[at], sems.at[2 * half + n])
            for n, (source, target) in enumerate(((genotype_ref, dosage_in), (mask_ref, mask_in)))
        ])
    for copy in copies[0] + copies[1]:
        copy.start()
    totals = []
    for half, part_ref in enumerate((first_ref, second_ref)):
        for copy in copies[half]:
            copy.wait()
        at = pl.ds(half * rows, rows)
        mask = mask_in[at, :]
        dosage = mask * dosage_in[at, :]
        calls = (dosage + mask).astype(jnp.float32).astype(jnp.bfloat16)
        whole_ref[at, :] = calls
        part_ref[...] = calls
        totals.append([
            jnp.sum(value.astype(jnp.float32), axis=0, keepdims=True) for value in (dosage, mask)
        ])
    for n in range(2):
        sums_ref[n : n + 1, :] = totals[0][n] + totals[1][n]


def encode(genotype, mask):
    rows, columns = genotype.shape
    half = rows // 2
    calls = lambda n: jax.ShapeDtypeStruct((n, columns), jnp.bfloat16)
    return pl.pallas_call(
        encode_body,
        name="encode",
        out_shape=(calls(rows), calls(half), calls(half), jax.ShapeDtypeStruct((2, columns), jnp.float32)),
        in_specs=[ANY, ANY],
        out_specs=(VMEM,) * 4,
        scratch_shapes=[
            pltpu.VMEM((rows, columns), jnp.int32),
            pltpu.VMEM((rows, columns), jnp.int32),
            pltpu.SemaphoreType.DMA((4,)),
        ],
        compiler_params=pltpu.CompilerParams(vmem_limit_bytes=40 * 2**20),
    )(pltpu.with_memory_space_constraint(genotype, pltpu.HBM), pltpu.with_memory_space_constraint(mask, pltpu.HBM))


def factors(sums):
    frequency = (sums[0:1] + 1.0) / (2.0 * sums[1:2] + 2.0)
    return 1.0 + 2.0 * frequency, 1.0 / jnp.sqrt(2.0 * frequency * (1.0 - frequency))


def standardized(calls, shift, scale):
    wide = calls.astype(jnp.float32)
    return jnp.where(wide > 0.0, (wide - shift) * scale, 0.0).astype(jnp.bfloat16)


def left_body(calls_ref, sums_ref, more_ref, left_ref, factors_ref):
    shift, scale = factors(sums_ref[...] + more_ref[...])
    factors_ref[0:1, :] = shift
    factors_ref[1:2, :] = scale
    left_ref[...] = standardized(calls_ref[...], shift, scale)


def multiply(left, right):
    return lax.dot_general(
        left, right, (((1,), (1,)), ((), ())), preferred_element_type=jnp.float32
    )


def products_body(cases, down, left_ref, factors_ref, *rest):
    *refs, keep_ref, away_ref, right_ref = rest
    shift, scale = factors_ref[0:1, :], factors_ref[1:2, :]
    device = lax.axis_index("snps")
    parity = lax.axis_index("samples") % 2
    for strip, by_parity in cases:
        for odd, (at, begin) in enumerate(by_parity):

            def fill(at=at, begin=begin):
                rows = refs[at][pl.ds(begin, right_ref.shape[0]), :]
                right_ref[...] = standardized(rows, shift, scale)

            if by_parity[0] != by_parity[1]:
                pl.when(parity == odd)(fill)
            elif not odd:
                fill()
        place = device ^ strip
        for bit, target_ref in enumerate((keep_ref, away_ref)):

            @pl.when(place % 2 == bit)
            def _(target_ref=target_ref, place=place):
                target_ref[place // 2] = multiply(left_ref[...], right_ref[...]) * down


def products_more_body(cases, down, left_ref, factors_ref, *rest):
    *refs, _, _, keep_ref, away_ref, right_ref = rest
    products_body(cases, down, left_ref, factors_ref, *refs, keep_ref, away_ref, right_ref)


def add_body(places, up, ours_ref, got_ref, *rest):
    out_ref, total_ref, sem = rest[-3:]
    total_ref[...] = (ours_ref[...] + got_ref[...]) * up
    device = lax.axis_index("snps")
    width = total_ref.shape[1]
    for strip, begin in enumerate(places):

        @pl.when(device == strip)
        def _(begin=begin):
            copy = pltpu.make_async_copy(total_ref, out_ref.at[:, pl.ds(begin, width)], sem)
            copy.start()
            copy.wait()


def per_device(genotype, mask):
    samples = lax.axis_size("samples")
    parts = lax.axis_size("snps")
    assert samples % 4 == 0 and samples & (samples - 1) == 0 and parts == 4
    rows, snp_part = genotype.shape
    snp_total = snp_part * parts
    turns = samples // 4
    half_rows = rows // 2
    width = rows * (samples // 2 + 1) // parts

    calls, first, second, sums = encode(genotype, mask)

    along = lambda s: (s - 2) % samples
    even = lax.axis_index("samples") % 2 == 0
    line = [[first, second]]
    for _ in range(1, turns + 1):
        line.append([send(line[-1][h], "samples", along) for h in range(2)])
    side = [None] + [[send(line[t][h], "samples", lambda s: s ^ 1) for h in range(2)] for t in range(1, turns)]
    side.append([send(jnp.where(even, line[turns][h], line[0][1 - h]), "samples", lambda s: s ^ 1) for h in range(2)])

    for bit in range(samples.bit_length() - 1):
        more = send(sums, "samples", lambda s, step=1 << bit: s ^ step)
        if 2 << bit < samples:
            sums = sums + more

    def source(k, h, odd):
        if k == 0:
            return calls, h * half_rows
        if k % 2 == 0:
            return line[k // 2][h], 0
        if k == 1 and not odd:
            return side[turns][1 - h], 0
        return side[(k + odd) // 2][h], 0

    left, pair = call_kernel(
        left_body,
        (jax.ShapeDtypeStruct((rows, snp_part), jnp.bfloat16), jax.ShapeDtypeStruct((2, snp_part), jnp.float32)),
        (calls, sums, more), [VMEM] * 3, 5 * rows * snp_part, 4 * rows * snp_part, out_specs=(VMEM, VMEM),
    )
    table = strips(samples)
    bound = snp_total / 2 * 4 * (samples * rows + 1) / 3
    down = 2.0 ** -math.ceil(math.log2(bound / 32768.0))
    count = len(table[0][0])
    quarter = half_rows // 2

    def products(n, chosen, so_far):
        columns = half_rows if n < count else quarter
        arrays, cases = [], []
        for strip in chosen:
            by_arrival, _, cut = table[strip]
            by_parity = []
            for odd in range(2):
                array, begin = source(*(by_arrival[n] if n < count else cut), odd)
                at = next((i for i, known in enumerate(arrays) if known is array), len(arrays))
                if at == len(arrays):
                    arrays.append(array)
                if n == count and strip % 2:
                    begin += quarter
                by_parity.append((at, begin))
            cases.append((strip, tuple(by_parity)))
        shape = jax.ShapeDtypeStruct((2, rows, columns), jnp.float32)
        operands = (left, pair, *arrays, *so_far)
        return call_kernel(
            functools.partial(products_body if not so_far else products_more_body, tuple(cases), down),
            (shape, shape), operands, [VMEM] * len(operands),
            2 * rows * snp_part * columns * len(chosen), 4 * rows * columns,
            out_specs=(VMEM, VMEM),
            scratch_shapes=[pltpu.VMEM((columns, snp_part), jnp.bfloat16)],
            input_output_aliases={len(operands) - 2 + i: i for i in range(len(so_far))},
        )

    pieces = []
    for n in range(count + 1):
        last_in = (1, 2 * turns - 1) + ((2 * turns,) if n == 0 else ())
        late = [
            strip for strip, (by_arrival, _, cut) in enumerate(table)
            if (by_arrival[n] if n < count else cut)[0] in last_in
        ]
        both = ()
        for chosen in ([s for s in range(4) if s not in late], late):
            if chosen:
                both = products(n, chosen, both)
        keep, away = both
        summed = keep + swap_core(away.astype(jnp.float16)).astype(jnp.float32)
        got = send(summed[1].astype(jnp.float16), "snps", lambda s: s ^ 2)
        pieces.append((summed[0], got.astype(jnp.float32)))
    out = None
    for n, operands in enumerate(pieces):
        places = []
        for strip, (by_arrival, natural, _) in enumerate(table):
            if n < count:
                places.append(natural.index(by_arrival[n]) * half_rows + (strip % 2) * quarter)
            else:
                places.append(0 if strip % 2 else count * half_rows)
        columns = operands[1].shape[1]
        last = () if out is None else (out,)
        operands = (*operands, *last)
        out = call_kernel(
            functools.partial(add_body, tuple(places), 1.0 / (down * snp_total)),
            jax.ShapeDtypeStruct((rows, width), jnp.float32), operands,
            [VMEM] * 2 + [ANY] * len(last), rows * columns, 4 * rows * columns,
            out_specs=ANY,
            scratch_shapes=[pltpu.VMEM((rows, columns), jnp.float32), pltpu.SemaphoreType.DMA],
            input_output_aliases={len(operands) - 1: 0} if last else {},
        )
    return out


def solution(mesh):
    return jax.shard_map(
        per_device,
        mesh=mesh,
        in_specs=(P("samples", "snps"), P("samples", "snps")),
        out_specs=P("samples", "snps"),
        check_vma=False,
    )
```

```python
import functools
import math

import jax
import jax.numpy as jnp
from jax import lax
from jax.experimental import pallas as pl
from jax.experimental.pallas import tpu as pltpu
from jax.sharding import PartitionSpec as P


def send(value, axis, route):
    count = lax.axis_size(axis)
    pairs = [(source, route(source)) for source in range(count)]
    return lax.ppermute(value, axis, [pair for pair in pairs if pair[1] is not None])


def swap_core(value):
    return send(value, "snps", lambda s: s ^ 1)


def arrival(piece):
    k, half = piece
    return k + 0.5 * half + (1.6 if k % 2 else 0.0)


def strips(samples):
    whole_count = (samples + 2) // 4
    result = []
    for strip in range(4):
        first = strip * (samples + 2) // 4
        begin = first + strip % 2
        wholes = [divmod(begin + n, 2) for n in range(whole_count)]
        cut = divmod(first if strip % 2 else first + whole_count, 2)
        result.append((sorted(wholes, key=arrival), wholes, cut))
    return result


def call_kernel(body, shapes, operands, specs, flops, moved, **more):
    return pl.pallas_call(
        body,
        out_shape=shapes,
        in_specs=specs,
        compiler_params=pltpu.CompilerParams(vmem_limit_bytes=24 * 2**20),
        cost_estimate=pl.CostEstimate(flops=flops, bytes_accessed=moved, transcendentals=0),
        **more,
    )(*operands)


VMEM = pl.BlockSpec(memory_space=pltpu.VMEM)
ANY = pl.BlockSpec(memory_space=pl.ANY)


def encode_body(genotype_ref, mask_ref, whole_ref, first_ref, second_ref, sums_ref,
                dosage_in, mask_in, sems):
    rows = first_ref.shape[0]
    copies = []
    for half in range(2):
        at = pl.ds(half * rows, rows)
        copies.append([
            pltpu.make_async_copy(source.at[at], target.at[at], sems.at[2 * half + n])
            for n, (source, target) in enumerate(((genotype_ref, dosage_in), (mask_ref, mask_in)))
        ])
    for copy in copies[0] + copies[1]:
        copy.start()
    totals = []
    for half, part_ref in enumerate((first_ref, second_ref)):
        for copy in copies[half]:
            copy.wait()
        at = pl.ds(half * rows, rows)
        mask = mask_in[at, :]
        dosage = mask * dosage_in[at, :]
        calls = (dosage + mask).astype(jnp.float32).astype(jnp.bfloat16)
        whole_ref[at, :] = calls
        part_ref[...] = calls
        totals.append([
            jnp.sum(value.astype(jnp.float32), axis=0, keepdims=True) for value in (dosage, mask)
        ])
    for n in range(2):
        sums_ref[n : n + 1, :] = totals[0][n] + totals[1][n]


def encode(genotype, mask):
    rows, columns = genotype.shape
    half = rows // 2
    calls = lambda n: jax.ShapeDtypeStruct((n, columns), jnp.bfloat16)
    return pl.pallas_call(
        encode_body,
        name="encode",
        out_shape=(calls(rows), calls(half), calls(half), jax.ShapeDtypeStruct((2, columns), jnp.float32)),
        in_specs=[ANY, ANY],
        out_specs=(VMEM,) * 4,
        scratch_shapes=[
            pltpu.VMEM((rows, columns), jnp.int32),
            pltpu.VMEM((rows, columns), jnp.int32),
            pltpu.SemaphoreType.DMA((4,)),
        ],
        compiler_params=pltpu.CompilerParams(vmem_limit_bytes=40 * 2**20),
    )(pltpu.with_memory_space_constraint(genotype, pltpu.HBM), pltpu.with_memory_space_constraint(mask, pltpu.HBM))


def factors(sums):
    frequency = (sums[0:1] + 1.0) / (2.0 * sums[1:2] + 2.0)
    return 1.0 + 2.0 * frequency, 1.0 / jnp.sqrt(2.0 * frequency * (1.0 - frequency))


def standardized(calls, shift, scale):
    wide = calls.astype(jnp.float32)
    return jnp.where(wide > 0.0, (wide - shift) * scale, 0.0).astype(jnp.bfloat16)


def left_body(calls_ref, sums_ref, more_ref, left_ref, factors_ref):
    shift, scale = factors(sums_ref[...] + more_ref[...])
    factors_ref[0:1, :] = shift
    factors_ref[1:2, :] = scale
    left_ref[...] = standardized(calls_ref[...], shift, scale)


def multiply(left, right):
    return lax.dot_general(
        left, right, (((1,), (1,)), ((), ())), preferred_element_type=jnp.float32
    )


def products_body(cases, down, left_ref, factors_ref, *rest):
    *refs, keep_ref, away_ref, right_ref = rest
    shift, scale = factors_ref[0:1, :], factors_ref[1:2, :]
    device = lax.axis_index("snps")
    parity = lax.axis_index("samples") % 2
    for strip, by_parity in cases:
        for odd, (at, begin) in enumerate(by_parity):

            def fill(at=at, begin=begin):
                rows = refs[at][pl.ds(begin, right_ref.shape[0]), :]
                right_ref[...] = standardized(rows, shift, scale)

            if by_parity[0] != by_parity[1]:
                pl.when(parity == odd)(fill)
            elif not odd:
                fill()
        place = device ^ strip
        for bit, target_ref in enumerate((keep_ref, away_ref)):

            @pl.when(place % 2 == bit)
            def _(target_ref=target_ref, place=place):
                target_ref[place // 2] = multiply(left_ref[...], right_ref[...]) * down


def products_more_body(cases, down, left_ref, factors_ref, *rest):
    *refs, _, _, keep_ref, away_ref, right_ref = rest
    products_body(cases, down, left_ref, factors_ref, *refs, keep_ref, away_ref, right_ref)


def add_body(places, up, ours_ref, got_ref, *rest):
    out_ref, total_ref, sem = rest[-3:]
    total_ref[...] = (ours_ref[...] + got_ref[...]) * up
    device = lax.axis_index("snps")
    width = total_ref.shape[1]
    for strip, begin in enumerate(places):

        @pl.when(device == strip)
        def _(begin=begin):
            copy = pltpu.make_async_copy(total_ref, out_ref.at[:, pl.ds(begin, width)], sem)
            copy.start()
            copy.wait()


def per_device(genotype, mask):
    samples = lax.axis_size("samples")
    parts = lax.axis_size("snps")
    assert samples % 4 == 0 and samples & (samples - 1) == 0 and parts == 4
    rows, snp_part = genotype.shape
    snp_total = snp_part * parts
    turns = samples // 4
    half_rows = rows // 2
    width = rows * (samples // 2 + 1) // parts

    calls, first, second, sums = encode(genotype, mask)

    along = lambda s: (s - 2) % samples
    even = lax.axis_index("samples") % 2 == 0
    line = [[first, second]]
    for _ in range(1, turns + 1):
        line.append([send(line[-1][h], "samples", along) for h in range(2)])
    side = [None] + [[send(line[t][h], "samples", lambda s: s ^ 1) for h in range(2)] for t in range(1, turns)]
    side.append([])
    for h in range(2):
        chosen = jnp.where(even, line[turns][h], line[0][1 - h])
        side[turns].append(send(chosen, "samples", lambda s: s ^ 1))

    for bit in range(samples.bit_length() - 1):
        more = send(sums, "samples", lambda s, step=1 << bit: s ^ step)
        if 2 << bit < samples:
            sums = sums + more

    def source(k, h, odd):
        if k == 0:
            return calls, h * half_rows
        if k % 2 == 0:
            return line[k // 2][h], 0
        if k == 1 and not odd:
            return side[turns][1 - h], 0
        return side[(k + odd) // 2][h], 0

    left, pair = call_kernel(
        left_body,
        (jax.ShapeDtypeStruct((rows, snp_part), jnp.bfloat16), jax.ShapeDtypeStruct((2, snp_part), jnp.float32)),
        (calls, sums, more), [VMEM] * 3, 5 * rows * snp_part, 4 * rows * snp_part, out_specs=(VMEM, VMEM),
    )
    table = strips(samples)
    bound = snp_total / 2 * 4 * (samples * rows + 1) / 3
    down = 2.0 ** -math.ceil(math.log2(bound / 32768.0))
    count = len(table[0][0])
    quarter = half_rows // 2

    def products(n, chosen, so_far):
        columns = half_rows if n < count else quarter
        arrays, cases = [], []
        for strip in chosen:
            by_arrival, _, cut = table[strip]
            by_parity = []
            for odd in range(2):
                array, begin = source(*(by_arrival[n] if n < count else cut), odd)
                at = next((i for i, known in enumerate(arrays) if known is array), len(arrays))
                if at == len(arrays):
                    arrays.append(array)
                if n == count and strip % 2:
                    begin += quarter
                by_parity.append((at, begin))
            cases.append((strip, tuple(by_parity)))
        shape = jax.ShapeDtypeStruct((2, rows, columns), jnp.float32)
        operands = (left, pair, *arrays, *so_far)
        return call_kernel(
            functools.partial(products_body if not so_far else products_more_body, tuple(cases), down),
            (shape, shape), operands, [VMEM] * len(operands),
            2 * rows * snp_part * columns * len(chosen), 4 * rows * columns,
            out_specs=(VMEM, VMEM),
            scratch_shapes=[pltpu.VMEM((columns, snp_part), jnp.bfloat16)],
            input_output_aliases={len(operands) - 2 + i: i for i in range(len(so_far))},
        )

    pieces = []
    for n in range(count + 1):
        last_in = (1, 2 * turns - 1) + ((2 * turns,) if n == 0 else ())
        late = [
            strip for strip, (by_arrival, _, cut) in enumerate(table)
            if (by_arrival[n] if n < count else cut)[0] in last_in
        ]
        both = ()
        for chosen in ([s for s in range(4) if s not in late], late):
            if chosen:
                both = products(n, chosen, both)
        keep, away = both
        summed = keep + swap_core(away.astype(jnp.float16)).astype(jnp.float32)
        got = send(summed[1].astype(jnp.float16), "snps", lambda s: s ^ 2)
        pieces.append((summed[0], got.astype(jnp.float32)))
    out = None
    for n, operands in enumerate(pieces):
        places = []
        for strip, (by_arrival, natural, _) in enumerate(table):
            if n < count:
                places.append(natural.index(by_arrival[n]) * half_rows + (strip % 2) * quarter)
            else:
                places.append(0 if strip % 2 else count * half_rows)
        columns = operands[1].shape[1]
        last = () if out is None else (out,)
        operands = (*operands, *last)
        out = call_kernel(
            functools.partial(add_body, tuple(places), 1.0 / (down * snp_total)),
            jax.ShapeDtypeStruct((rows, width), jnp.float32), operands,
            [VMEM] * 2 + [ANY] * len(last), rows * columns, 4 * rows * columns,
            out_specs=ANY,
            scratch_shapes=[pltpu.VMEM((rows, columns), jnp.float32), pltpu.SemaphoreType.DMA],
            input_output_aliases={len(operands) - 1: 0} if last else {},
        )
    return out


def solution(mesh):
    return jax.shard_map(
        per_device,
        mesh=mesh,
        in_specs=(P("samples", "snps"), P("samples", "snps")),
        out_specs=P("samples", "snps"),
        check_vma=False,
    )
```

```python
import functools
import math

import jax
import jax.numpy as jnp
from jax import lax
from jax.experimental import pallas as pl
from jax.experimental.pallas import tpu as pltpu
from jax.sharding import PartitionSpec as P


def send(value, axis, route):
    count = lax.axis_size(axis)
    pairs = [(source, route(source)) for source in range(count)]
    return lax.ppermute(value, axis, [pair for pair in pairs if pair[1] is not None])


def swap_core(value):
    return send(value, "snps", lambda s: s ^ 1)


def arrival(piece):
    k, half = piece
    return k + 0.5 * half + (1.6 if k % 2 else 0.0)


def strips(samples):
    whole_count = (samples + 2) // 4
    result = []
    for strip in range(4):
        first = strip * (samples + 2) // 4
        begin = first + strip % 2
        wholes = [divmod(begin + n, 2) for n in range(whole_count)]
        cut = divmod(first if strip % 2 else first + whole_count, 2)
        result.append((sorted(wholes, key=arrival), wholes, cut))
    return result


def call_kernel(body, shapes, operands, specs, flops, moved, **more):
    return pl.pallas_call(
        body,
        out_shape=shapes,
        in_specs=specs,
        compiler_params=pltpu.CompilerParams(vmem_limit_bytes=12 * 2**20),
        cost_estimate=pl.CostEstimate(flops=flops, bytes_accessed=moved, transcendentals=0),
        **more,
    )(*operands)


VMEM = pl.BlockSpec(memory_space=pltpu.VMEM)
ANY = pl.BlockSpec(memory_space=pl.ANY)


def encode_body(genotype_ref, mask_ref, whole_ref, first_ref, second_ref, sums_ref,
                dosage_in, mask_in, sems):
    rows = first_ref.shape[0]
    copies = []
    for half in range(2):
        at = pl.ds(half * rows, rows)
        copies.append([
            pltpu.make_async_copy(source.at[at], target.at[at], sems.at[2 * half + n])
            for n, (source, target) in enumerate(((genotype_ref, dosage_in), (mask_ref, mask_in)))
        ])
    for copy in copies[0] + copies[1]:
        copy.start()
    totals = []
    for half, part_ref in enumerate((first_ref, second_ref)):
        for copy in copies[half]:
            copy.wait()
        at = pl.ds(half * rows, rows)
        mask = mask_in[at, :]
        dosage = mask * dosage_in[at, :]
        calls = (dosage + mask).astype(jnp.float32).astype(jnp.bfloat16)
        whole_ref[at, :] = calls
        part_ref[...] = calls
        totals.append([
            jnp.sum(value.astype(jnp.float32), axis=0, keepdims=True) for value in (dosage, mask)
        ])
    for n in range(2):
        sums_ref[n : n + 1, :] = totals[0][n] + totals[1][n]


def encode(genotype, mask):
    rows, columns = genotype.shape
    half = rows // 2
    calls = lambda n: jax.ShapeDtypeStruct((n, columns), jnp.bfloat16)
    return pl.pallas_call(
        encode_body,
        name="encode",
        out_shape=(calls(rows), calls(half), calls(half), jax.ShapeDtypeStruct((2, columns), jnp.float32)),
        in_specs=[ANY, ANY],
        out_specs=(VMEM,) * 4,
        scratch_shapes=[
            pltpu.VMEM((rows, columns), jnp.int32),
            pltpu.VMEM((rows, columns), jnp.int32),
            pltpu.SemaphoreType.DMA((4,)),
        ],
        compiler_params=pltpu.CompilerParams(vmem_limit_bytes=40 * 2**20),
    )(pltpu.with_memory_space_constraint(genotype, pltpu.HBM), pltpu.with_memory_space_constraint(mask, pltpu.HBM))


def factors(sums):
    frequency = (sums[0:1] + 1.0) / (2.0 * sums[1:2] + 2.0)
    return 1.0 + 2.0 * frequency, 1.0 / jnp.sqrt(2.0 * frequency * (1.0 - frequency))


def standardized(calls, shift, scale):
    wide = calls.astype(jnp.float32)
    return jnp.where(wide > 0.0, (wide - shift) * scale, 0.0).astype(jnp.bfloat16)


def left_body(calls_ref, sums_ref, more_ref, left_ref, factors_ref):
    shift, scale = factors(sums_ref[...] + more_ref[...])
    factors_ref[0:1, :] = shift
    factors_ref[1:2, :] = scale
    left_ref[...] = standardized(calls_ref[...], shift, scale)


def multiply(left, right):
    return lax.dot_general(
        left, right, (((1,), (1,)), ((), ())), preferred_element_type=jnp.float32
    )


def products_body(cases, down, left_ref, factors_ref, *rest):
    refs, target_refs, right_ref = rest[:-5], rest[-5:-1], rest[-1]
    shift, scale = factors_ref[0:1, :], factors_ref[1:2, :]
    device = lax.axis_index("snps")
    parity = lax.axis_index("samples") % 2
    for strip, at, begin, only in cases:

        def work(strip=strip, at=at, begin=begin):
            rows = refs[at][pl.ds(begin, right_ref.shape[0]), :]
            right_ref[...] = standardized(rows, shift, scale)
            place = device ^ strip
            for index, target_ref in enumerate(target_refs):

                @pl.when(place == index)
                def _(target_ref=target_ref):
                    target_ref[...] = multiply(left_ref[...], right_ref[...]) * down

        if only is None:
            work()
        else:
            pl.when(parity == only)(work)


def products_more_body(cases, down, left_ref, factors_ref, *rest):
    products_body(cases, down, left_ref, factors_ref, *rest[:-9], *rest[-5:])


def add_body(places, up, ours_ref, got_ref, *rest):
    out_ref, total_ref, sem = rest[-3:]
    total_ref[...] = (ours_ref[...] + got_ref[...]) * up
    device = lax.axis_index("snps")
    width = total_ref.shape[1]
    for strip, begin in enumerate(places):

        @pl.when(device == strip)
        def _(begin=begin):
            copy = pltpu.make_async_copy(total_ref, out_ref.at[:, pl.ds(begin, width)], sem)
            copy.start()
            copy.wait()


def per_device(genotype, mask):
    samples = lax.axis_size("samples")
    parts = lax.axis_size("snps")
    assert samples % 4 == 0 and samples & (samples - 1) == 0 and parts == 4
    rows, snp_part = genotype.shape
    snp_total = snp_part * parts
    turns = samples // 4
    half_rows = rows // 2
    width = rows * (samples // 2 + 1) // parts

    calls, first, second, sums = encode(genotype, mask)

    along = lambda s: (s - 2) % samples
    even = lax.axis_index("samples") % 2 == 0
    line = [[first, second]]
    for _ in range(1, turns + 1):
        line.append([send(line[-1][h], "samples", along) for h in range(2)])
    side = [None] + [[send(line[t][h], "samples", lambda s: s ^ 1) for h in range(2)] for t in range(1, turns)]
    side.append([])
    for h in range(2):
        chosen = jnp.where(even, line[turns][h], line[0][1 - h])
        side[turns].append(send(chosen, "samples", lambda s: s ^ 1))

    for bit in range(samples.bit_length() - 1):
        more = send(sums, "samples", lambda s, step=1 << bit: s ^ step)
        if 2 << bit < samples:
            sums = sums + more

    def source(k, h, odd):
        if k == 0:
            return calls, h * half_rows
        if k % 2 == 0:
            return line[k // 2][h], 0
        if k == 1 and not odd:
            return side[turns][1 - h], 0
        return side[(k + odd) // 2][h], 0

    left, pair = call_kernel(
        left_body,
        (jax.ShapeDtypeStruct((rows, snp_part), jnp.bfloat16), jax.ShapeDtypeStruct((2, snp_part), jnp.float32)),
        (calls, sums, more), [VMEM] * 3, 5 * rows * snp_part, 4 * rows * snp_part, out_specs=(VMEM, VMEM),
    )
    table = strips(samples)
    bound = snp_total / 2 * 4 * (samples * rows + 1) / 3
    down = 2.0 ** -math.ceil(math.log2(bound / 32768.0))
    count = len(table[0][0])
    quarter = half_rows // 2

    def sources(n):
        result = []
        for strip, (by_arrival, _, cut) in enumerate(table):
            k, h = by_arrival[n] if n < count else cut
            shift_rows = quarter if n == count and strip % 2 else 0
            for odd in range(2):
                array, begin = source(k, h, odd)
                last = (2 * turns - 1 if odd else 1) if k % 2 else (2 * turns if n == 0 else -1)
                result.append((strip, array, begin + shift_rows, odd if k % 2 else None, k == last))
                if k % 2 == 0:
                    break
        return result

    def products(columns, chosen, so_far):
        arrays, cases = [], []
        for strip, array, begin, only, _ in chosen:
            at = next((i for i, known in enumerate(arrays) if known is array), len(arrays))
            if at == len(arrays):
                arrays.append(array)
            cases.append((strip, at, begin, only))
        shape = jax.ShapeDtypeStruct((rows, columns), jnp.float32)
        operands = (left, pair, *arrays, *so_far)
        return call_kernel(
            functools.partial(products_body if not so_far else products_more_body, tuple(cases), down),
            (shape,) * 4, operands, [VMEM] * len(operands),
            2 * rows * snp_part * columns * len(chosen), 4 * rows * columns,
            out_specs=(VMEM,) * 4,
            scratch_shapes=[pltpu.VMEM((columns, snp_part), jnp.bfloat16)],
            input_output_aliases={len(operands) - 4 + i: i for i in range(len(so_far))},
        )

    pieces, partners = [], []
    for n in range(count + 1):
        columns = half_rows if n < count else quarter
        both = ()
        for wanted in (False, True):
            chosen = [entry for entry in sources(n) if entry[-1] == wanted]
            if chosen:
                both = products(columns, chosen, both)
        own, own_away, neighbour, neighbour_away = both
        other = swap_core(neighbour_away.astype(jnp.float16))
        theirs = (neighbour + other.astype(jnp.float32)).astype(jnp.float16)
        pieces.append((own, send(theirs, "snps", lambda s: s ^ 2)))
        partners.append(own_away.astype(jnp.float16))
    other = swap_core(jnp.concatenate(partners, axis=1))
    for n, (keep, got) in enumerate(pieces):
        begin = n * half_rows
        ours = keep + other[:, begin : begin + keep.shape[1]].astype(jnp.float32)
        pieces[n] = (ours, got.astype(jnp.float32))
    out = None
    for n, operands in enumerate(pieces):
        places = []
        for strip, (by_arrival, natural, _) in enumerate(table):
            if n < count:
                places.append(natural.index(by_arrival[n]) * half_rows + (strip % 2) * quarter)
            else:
                places.append(0 if strip % 2 else count * half_rows)
        columns = operands[1].shape[1]
        last = () if out is None else (out,)
        operands = (*operands, *last)
        out = call_kernel(
            functools.partial(add_body, tuple(places), 1.0 / (down * snp_total)),
            jax.ShapeDtypeStruct((rows, width), jnp.float32), operands,
            [VMEM] * 2 + [ANY] * len(last), rows * columns, 4 * rows * columns,
            out_specs=ANY,
            scratch_shapes=[pltpu.VMEM((rows, columns), jnp.float32), pltpu.SemaphoreType.DMA],
            input_output_aliases={len(operands) - 1: 0} if last else {},
        )
    return out


def solution(mesh):
    return jax.shard_map(
        per_device,
        mesh=mesh,
        in_specs=(P("samples", "snps"), P("samples", "snps")),
        out_specs=P("samples", "snps"),
        check_vma=False,
    )
```

```python
import functools
import math

import jax
import jax.numpy as jnp
from jax import lax
from jax.experimental import pallas as pl
from jax.experimental.pallas import tpu as pltpu
from jax.sharding import PartitionSpec as P


def send(value, axis, route):
    count = lax.axis_size(axis)
    pairs = [(source, route(source)) for source in range(count)]
    return lax.ppermute(value, axis, [pair for pair in pairs if pair[1] is not None])


def swap_core(value):
    return send(value, "snps", lambda s: s ^ 1)


def arrival(piece):
    k, half = piece
    return k + 0.5 * half + (1.6 if k % 2 else 0.0)


def strips(samples):
    whole_count = (samples + 2) // 4
    result = []
    for strip in range(4):
        first = strip * (samples + 2) // 4
        begin = first + strip % 2
        wholes = [divmod(begin + n, 2) for n in range(whole_count)]
        cut = divmod(first if strip % 2 else first + whole_count, 2)
        result.append((sorted(wholes, key=arrival), wholes, cut))
    return result


def call_kernel(body, shapes, operands, specs, flops, moved, **more):
    return pl.pallas_call(
        body,
        out_shape=shapes,
        in_specs=specs,
        compiler_params=pltpu.CompilerParams(vmem_limit_bytes=12 * 2**20),
        cost_estimate=pl.CostEstimate(flops=flops, bytes_accessed=moved, transcendentals=0),
        **more,
    )(*operands)


VMEM = pl.BlockSpec(memory_space=pltpu.VMEM)
ANY = pl.BlockSpec(memory_space=pl.ANY)


def encode_body(genotype_ref, mask_ref, whole_ref, first_ref, second_ref, sums_ref,
                dosage_in, mask_in, sems):
    rows = first_ref.shape[0]
    copies = []
    for half in range(2):
        at = pl.ds(half * rows, rows)
        copies.append([
            pltpu.make_async_copy(source.at[at], target.at[at], sems.at[2 * half + n])
            for n, (source, target) in enumerate(((genotype_ref, dosage_in), (mask_ref, mask_in)))
        ])
    for copy in copies[0] + copies[1]:
        copy.start()
    totals = []
    for half, part_ref in enumerate((first_ref, second_ref)):
        for copy in copies[half]:
            copy.wait()
        at = pl.ds(half * rows, rows)
        mask = mask_in[at, :]
        dosage = mask * dosage_in[at, :]
        calls = (dosage + mask).astype(jnp.float32).astype(jnp.bfloat16)
        whole_ref[at, :] = calls
        part_ref[...] = calls
        totals.append([
            jnp.sum(value.astype(jnp.float32), axis=0, keepdims=True) for value in (dosage, mask)
        ])
    for n in range(2):
        sums_ref[n : n + 1, :] = totals[0][n] + totals[1][n]


def encode(genotype, mask):
    rows, columns = genotype.shape
    half = rows // 2
    calls = lambda n: jax.ShapeDtypeStruct((n, columns), jnp.bfloat16)
    return pl.pallas_call(
        encode_body,
        name="encode",
        out_shape=(calls(rows), calls(half), calls(half), jax.ShapeDtypeStruct((2, columns), jnp.float32)),
        in_specs=[ANY, ANY],
        out_specs=(VMEM,) * 4,
        scratch_shapes=[
            pltpu.VMEM((rows, columns), jnp.int32),
            pltpu.VMEM((rows, columns), jnp.int32),
            pltpu.SemaphoreType.DMA((4,)),
        ],
        compiler_params=pltpu.CompilerParams(vmem_limit_bytes=40 * 2**20),
    )(pltpu.with_memory_space_constraint(genotype, pltpu.HBM), pltpu.with_memory_space_constraint(mask, pltpu.HBM))


def factors(sums):
    frequency = (sums[0:1] + 1.0) / (2.0 * sums[1:2] + 2.0)
    return 1.0 + 2.0 * frequency, 1.0 / jnp.sqrt(2.0 * frequency * (1.0 - frequency))


def standardized(calls, shift, scale):
    wide = calls.astype(jnp.float32)
    return jnp.where(wide > 0.0, (wide - shift) * scale, 0.0).astype(jnp.bfloat16)


def left_body(calls_ref, sums_ref, more_ref, left_ref, factors_ref):
    shift, scale = factors(sums_ref[...] + more_ref[...])
    factors_ref[0:1, :] = shift
    factors_ref[1:2, :] = scale
    left_ref[...] = standardized(calls_ref[...], shift, scale)


def multiply(left, right):
    return lax.dot_general(
        left, right, (((1,), (1,)), ((), ())), preferred_element_type=jnp.float32
    )


def products_body(cases, down, left_ref, factors_ref, *rest):
    refs, target_refs, right_ref = rest[:-5], rest[-5:-1], rest[-1]
    shift, scale = factors_ref[0:1, :], factors_ref[1:2, :]
    device = lax.axis_index("snps")
    parity = lax.axis_index("samples") % 2
    for strip, at, begin, only in cases:

        def work(strip=strip, at=at, begin=begin):
            rows = refs[at][pl.ds(begin, right_ref.shape[0]), :]
            right_ref[...] = standardized(rows, shift, scale)
            place = device ^ strip
            for index, target_ref in enumerate(target_refs):

                @pl.when(place == index)
                def _(target_ref=target_ref):
                    target_ref[...] = multiply(left_ref[...], right_ref[...]) * down

        if only is None:
            work()
        else:
            pl.when(parity == only)(work)


def products_more_body(cases, down, left_ref, factors_ref, *rest):
    products_body(cases, down, left_ref, factors_ref, *rest[:-9], *rest[-5:])


def add_body(places, at, up, ours_ref, got_ref, other_ref, *rest):
    out_ref, total_ref, sem = rest[-3:]
    other = other_ref[:, pl.ds(at, total_ref.shape[1])]
    total_ref[...] = (ours_ref[...] + other + got_ref[...]) * up
    device = lax.axis_index("snps")
    width = total_ref.shape[1]
    for strip, begin in enumerate(places):

        @pl.when(device == strip)
        def _(begin=begin):
            copy = pltpu.make_async_copy(total_ref, out_ref.at[:, pl.ds(begin, width)], sem)
            copy.start()
            copy.wait()


def per_device(genotype, mask):
    samples = lax.axis_size("samples")
    parts = lax.axis_size("snps")
    assert samples % 4 == 0 and samples & (samples - 1) == 0 and parts == 4
    rows, snp_part = genotype.shape
    snp_total = snp_part * parts
    turns = samples // 4
    half_rows = rows // 2
    width = rows * (samples // 2 + 1) // parts

    calls, first, second, sums = encode(genotype, mask)

    along = lambda s: (s - 2) % samples
    even = lax.axis_index("samples") % 2 == 0
    line = [[first, second]]
    for _ in range(1, turns + 1):
        line.append([send(line[-1][h], "samples", along) for h in range(2)])
    side = [None] + [[send(line[t][h], "samples", lambda s: s ^ 1) for h in range(2)] for t in range(1, turns)]
    side.append([])
    for h in range(2):
        chosen = jnp.where(even, line[turns][h], line[0][1 - h])
        side[turns].append(send(chosen, "samples", lambda s: s ^ 1))

    for bit in range(samples.bit_length() - 1):
        more = send(sums, "samples", lambda s, step=1 << bit: s ^ step)
        if 2 << bit < samples:
            sums = sums + more

    def source(k, h, odd):
        if k == 0:
            return calls, h * half_rows
        if k % 2 == 0:
            return line[k // 2][h], 0
        if k == 1 and not odd:
            return side[turns][1 - h], 0
        return side[(k + odd) // 2][h], 0

    left, pair = call_kernel(
        left_body,
        (jax.ShapeDtypeStruct((rows, snp_part), jnp.bfloat16), jax.ShapeDtypeStruct((2, snp_part), jnp.float32)),
        (calls, sums, more), [VMEM] * 3, 5 * rows * snp_part, 4 * rows * snp_part, out_specs=(VMEM, VMEM),
    )
    table = strips(samples)
    bound = snp_total / 2 * 4 * (samples * rows + 1) / 3
    down = 2.0 ** -math.ceil(math.log2(bound / 32768.0))
    count = len(table[0][0])
    quarter = half_rows // 2

    def sources(n):
        result = []
        for strip, (by_arrival, _, cut) in enumerate(table):
            k, h = by_arrival[n] if n < count else cut
            shift_rows = quarter if n == count and strip % 2 else 0
            for odd in range(2):
                array, begin = source(k, h, odd)
                last = (2 * turns - 1 if odd else 1) if k % 2 else (2 * turns if n == 0 else -1)
                result.append((strip, array, begin + shift_rows, odd if k % 2 else None, k == last))
                if k % 2 == 0:
                    break
        return result

    def products(columns, chosen, so_far):
        arrays, cases = [], []
        for strip, array, begin, only, _ in chosen:
            at = next((i for i, known in enumerate(arrays) if known is array), len(arrays))
            if at == len(arrays):
                arrays.append(array)
            cases.append((strip, at, begin, only))
        shape = jax.ShapeDtypeStruct((rows, columns), jnp.float32)
        operands = (left, pair, *arrays, *so_far)
        return call_kernel(
            functools.partial(products_body if not so_far else products_more_body, tuple(cases), down),
            (shape,) * 4, operands, [VMEM] * len(operands),
            2 * rows * snp_part * columns * len(chosen), 4 * rows * columns,
            out_specs=(VMEM,) * 4,
            scratch_shapes=[pltpu.VMEM((columns, snp_part), jnp.bfloat16)],
            input_output_aliases={len(operands) - 4 + i: i for i in range(len(so_far))},
        )

    pieces, partners = [], []
    for n in range(count + 1):
        columns = half_rows if n < count else quarter
        both = ()
        for wanted in (False, True):
            chosen = [entry for entry in sources(n) if entry[-1] == wanted]
            if chosen:
                both = products(columns, chosen, both)
        own, own_away, neighbour, neighbour_away = both
        other = swap_core(neighbour_away.astype(jnp.float16))
        theirs = (neighbour + other.astype(jnp.float32)).astype(jnp.float16)
        pieces.append((own, send(theirs, "snps", lambda s: s ^ 2)))
        partners.append(own_away.astype(jnp.float16))
    other = swap_core(jnp.concatenate(partners, axis=1)).astype(jnp.float32)
    out = None
    for n, operands in enumerate(pieces):
        places = []
        for strip, (by_arrival, natural, _) in enumerate(table):
            if n < count:
                places.append(natural.index(by_arrival[n]) * half_rows + (strip % 2) * quarter)
            else:
                places.append(0 if strip % 2 else count * half_rows)
        ours, got = operands
        columns = got.shape[1]
        last = () if out is None else (out,)
        operands = (ours, got.astype(jnp.float32), other, *last)
        out = call_kernel(
            functools.partial(add_body, tuple(places), n * half_rows, 1.0 / (down * snp_total)),
            jax.ShapeDtypeStruct((rows, width), jnp.float32), operands,
            [VMEM] * 3 + [ANY] * len(last), rows * columns, 4 * rows * columns,
            out_specs=ANY,
            scratch_shapes=[pltpu.VMEM((rows, columns), jnp.float32), pltpu.SemaphoreType.DMA],
            input_output_aliases={len(operands) - 1: 0} if last else {},
        )
    return out


def solution(mesh):
    return jax.shard_map(
        per_device,
        mesh=mesh,
        in_specs=(P("samples", "snps"), P("samples", "snps")),
        out_specs=P("samples", "snps"),
        check_vma=False,
    )
```

```python
import functools
import math

import jax
import jax.numpy as jnp
from jax import lax
from jax.experimental import pallas as pl
from jax.experimental.pallas import tpu as pltpu
from jax.sharding import PartitionSpec as P


def send(value, axis, route):
    count = lax.axis_size(axis)
    pairs = [(source, route(source)) for source in range(count)]
    return lax.ppermute(value, axis, [pair for pair in pairs if pair[1] is not None])


def swap_core(value):
    return send(value, "snps", lambda s: s ^ 1)


def arrival(piece):
    k, half = piece
    return k + 0.5 * half + (1.6 if k % 2 else 0.0)


def strips(samples):
    whole_count = (samples + 2) // 4
    result = []
    for strip in range(4):
        first = strip * (samples + 2) // 4
        begin = first + strip % 2
        wholes = [divmod(begin + n, 2) for n in range(whole_count)]
        cut = divmod(first if strip % 2 else first + whole_count, 2)
        result.append((sorted(wholes, key=arrival), wholes, cut))
    return result


def call_kernel(body, shapes, operands, specs, flops, moved, **more):
    return pl.pallas_call(
        body,
        out_shape=shapes,
        in_specs=specs,
        compiler_params=pltpu.CompilerParams(vmem_limit_bytes=12 * 2**20),
        cost_estimate=pl.CostEstimate(flops=flops, bytes_accessed=moved, transcendentals=0),
        **more,
    )(*operands)


VMEM = pl.BlockSpec(memory_space=pltpu.VMEM)
ANY = pl.BlockSpec(memory_space=pl.ANY)


def encode_body(genotype_ref, mask_ref, whole_ref, first_ref, second_ref, sums_ref,
                dosage_in, mask_in, sems):
    rows = first_ref.shape[0]
    copies = []
    for half in range(2):
        at = pl.ds(half * rows, rows)
        copies.append([
            pltpu.make_async_copy(source.at[at], target.at[at], sems.at[2 * half + n])
            for n, (source, target) in enumerate(((genotype_ref, dosage_in), (mask_ref, mask_in)))
        ])
    for copy in copies[0] + copies[1]:
        copy.start()
    totals = []
    for half, part_ref in enumerate((first_ref, second_ref)):
        for copy in copies[half]:
            copy.wait()
        at = pl.ds(half * rows, rows)
        mask = mask_in[at, :]
        dosage = mask * dosage_in[at, :]
        calls = (dosage + mask).astype(jnp.float32).astype(jnp.bfloat16)
        whole_ref[at, :] = calls
        part_ref[...] = calls
        totals.append([
            jnp.sum(value.astype(jnp.float32), axis=0, keepdims=True) for value in (dosage, mask)
        ])
    for n in range(2):
        sums_ref[n : n + 1, :] = totals[0][n] + totals[1][n]


def encode(genotype, mask):
    rows, columns = genotype.shape
    half = rows // 2
    calls = lambda n: jax.ShapeDtypeStruct((n, columns), jnp.bfloat16)
    return pl.pallas_call(
        encode_body,
        name="encode",
        out_shape=(calls(rows), calls(half), calls(half), jax.ShapeDtypeStruct((2, columns), jnp.float32)),
        in_specs=[ANY, ANY],
        out_specs=(VMEM,) * 4,
        scratch_shapes=[
            pltpu.VMEM((rows, columns), jnp.int32),
            pltpu.VMEM((rows, columns), jnp.int32),
            pltpu.SemaphoreType.DMA((4,)),
        ],
        compiler_params=pltpu.CompilerParams(vmem_limit_bytes=40 * 2**20),
    )(pltpu.with_memory_space_constraint(genotype, pltpu.HBM), pltpu.with_memory_space_constraint(mask, pltpu.HBM))


def factors(sums):
    frequency = (sums[0:1] + 1.0) / (2.0 * sums[1:2] + 2.0)
    return 1.0 + 2.0 * frequency, 1.0 / jnp.sqrt(2.0 * frequency * (1.0 - frequency))


def standardized(calls, shift, scale):
    wide = calls.astype(jnp.float32)
    return jnp.where(wide > 0.0, (wide - shift) * scale, 0.0).astype(jnp.bfloat16)


def left_body(down, calls_ref, sums_ref, more_ref, left_ref, factors_ref):
    shift, scale = factors(sums_ref[...] + more_ref[...])
    factors_ref[0:1, :] = shift
    factors_ref[1:2, :] = scale
    left_ref[...] = standardized(calls_ref[...], shift, scale) * down


def multiply(left, right):
    return lax.dot_general(
        left, right, (((1,), (1,)), ((), ())), preferred_element_type=jnp.float32
    )


def products_body(cases, left_ref, factors_ref, *rest):
    refs, target_refs, right_ref = rest[:-5], rest[-5:-1], rest[-1]
    shift, scale = factors_ref[0:1, :], factors_ref[1:2, :]
    parity = lax.axis_index("samples") % 2
    columns = right_ref.shape[1]

    def work(device, only):
        for n, (strip, at, begin, wanted) in enumerate(cases):
            if wanted == only:
                right_ref[n] = standardized(refs[at][pl.ds(begin, columns), :], shift, scale)
                target_refs[device ^ strip][...] = multiply(left_ref[...], right_ref[n])

    for device in range(len(target_refs)):

        @pl.when(lax.axis_index("snps") == device)
        def _(device=device):
            kinds = {wanted for *_, wanted in cases}
            if None in kinds:
                work(device, None)
            for odd in sorted(kinds - {None}):
                pl.when(parity == odd)(functools.partial(work, device, odd))


def products_more_body(cases, left_ref, factors_ref, *rest):
    products_body(cases, left_ref, factors_ref, *rest[:-9], *rest[-5:])


def add_body(places, at, up, ours_ref, got_ref, other_ref, *rest):
    out_ref, total_ref, sem = rest[-3:]
    other = other_ref[:, pl.ds(at, total_ref.shape[1])]
    total_ref[...] = (ours_ref[...] + other + got_ref[...]) * up
    device = lax.axis_index("snps")
    width = total_ref.shape[1]
    for strip, begin in enumerate(places):

        @pl.when(device == strip)
        def _(begin=begin):
            copy = pltpu.make_async_copy(total_ref, out_ref.at[:, pl.ds(begin, width)], sem)
            copy.start()
            copy.wait()


def per_device(genotype, mask):
    samples = lax.axis_size("samples")
    parts = lax.axis_size("snps")
    assert samples % 4 == 0 and samples & (samples - 1) == 0 and parts == 4
    rows, snp_part = genotype.shape
    snp_total = snp_part * parts
    turns = samples // 4
    half_rows = rows // 2
    width = rows * (samples // 2 + 1) // parts

    calls, first, second, sums = encode(genotype, mask)

    along = lambda s: (s - 2) % samples
    even = lax.axis_index("samples") % 2 == 0
    line = [[first, second]]
    for _ in range(1, turns + 1):
        line.append([send(line[-1][h], "samples", along) for h in range(2)])
    side = [None] + [
        [send(line[t][h], "samples", lambda s: s ^ 1) for h in range(2)]
        for t in range(1, turns)
    ]
    side.append([])
    for h in range(2):
        chosen = jnp.where(even, line[turns][h], line[0][1 - h])
        side[turns].append(send(chosen, "samples", lambda s: s ^ 1))

    for bit in range(samples.bit_length() - 1):
        more = send(sums, "samples", lambda s, step=1 << bit: s ^ step)
        if 2 << bit < samples:
            sums = sums + more

    def source(k, h, odd):
        if k == 0:
            return calls, h * half_rows
        if k % 2 == 0:
            return line[k // 2][h], 0
        if k == 1 and not odd:
            return side[turns][1 - h], 0
        return side[(k + odd) // 2][h], 0

    table = strips(samples)
    bound = snp_total / 2 * 4 * (samples * rows + 1) / 3
    down = 2.0 ** -math.ceil(math.log2(bound / 32768.0))
    left, pair = call_kernel(
        functools.partial(left_body, down),
        (jax.ShapeDtypeStruct((rows, snp_part), jnp.bfloat16), jax.ShapeDtypeStruct((2, snp_part), jnp.float32)),
        (calls, sums, more), [VMEM] * 3, 5 * rows * snp_part, 4 * rows * snp_part, out_specs=(VMEM, VMEM),
    )
    count = len(table[0][0])
    quarter = half_rows // 2

    def sources(n):
        result = []
        for strip, (by_arrival, _, cut) in enumerate(table):
            k, h = by_arrival[n] if n < count else cut
            shift_rows = quarter if n == count and strip % 2 else 0
            for odd in range(2):
                array, begin = source(k, h, odd)
                last = (2 * turns - 1 if odd else 1) if k % 2 else (2 * turns if n == 0 else -1)
                result.append((strip, array, begin + shift_rows, odd if k % 2 else None, k == last))
                if k % 2 == 0:
                    break
        return result

    def products(columns, chosen, so_far):
        arrays, cases = [], []
        for strip, array, begin, only, _ in chosen:
            at = next((i for i, known in enumerate(arrays) if known is array), len(arrays))
            if at == len(arrays):
                arrays.append(array)
            cases.append((strip, at, begin, only))
        shape = jax.ShapeDtypeStruct((rows, columns), jnp.float32)
        operands = (left, pair, *arrays, *so_far)
        return call_kernel(
            functools.partial(products_body if not so_far else products_more_body, tuple(cases)),
            (shape,) * 4, operands, [VMEM] * len(operands),
            2 * rows * snp_part * columns * len(chosen), 4 * rows * columns,
            out_specs=(VMEM,) * 4,
            scratch_shapes=[pltpu.VMEM((len(cases), columns, snp_part), jnp.bfloat16)],
            input_output_aliases={len(operands) - 4 + i: i for i in range(len(so_far))},
        )

    pieces, partners = [], []
    for n in range(count + 1):
        columns = half_rows if n < count else quarter
        both = ()
        for wanted in (False, True):
            chosen = [entry for entry in sources(n) if entry[-1] == wanted]
            if chosen:
                both = products(columns, chosen, both)
        own, own_away, neighbour, neighbour_away = both
        other = swap_core(neighbour_away.astype(jnp.float16))
        theirs = (neighbour + other.astype(jnp.float32)).astype(jnp.float16)
        pieces.append((own, send(theirs, "snps", lambda s: s ^ 2)))
        partners.append(own_away.astype(jnp.float16))
    other = swap_core(jnp.concatenate(partners, axis=1)).astype(jnp.float32)
    out = None
    for n, operands in enumerate(pieces):
        places = []
        for strip, (by_arrival, natural, _) in enumerate(table):
            if n < count:
                places.append(natural.index(by_arrival[n]) * half_rows + (strip % 2) * quarter)
            else:
                places.append(0 if strip % 2 else count * half_rows)
        ours, got = operands
        columns = got.shape[1]
        last = () if out is None else (out,)
        operands = (ours, got.astype(jnp.float32), other, *last)
        out = call_kernel(
            functools.partial(add_body, tuple(places), n * half_rows, 1.0 / (down * snp_total)),
            jax.ShapeDtypeStruct((rows, width), jnp.float32), operands,
            [VMEM] * 3 + [ANY] * len(last), rows * columns, 4 * rows * columns,
            out_specs=ANY,
            scratch_shapes=[pltpu.VMEM((rows, columns), jnp.float32), pltpu.SemaphoreType.DMA],
            input_output_aliases={len(operands) - 1: 0} if last else {},
        )
    return out


def solution(mesh):
    return jax.shard_map(
        per_device,
        mesh=mesh,
        in_specs=(P("samples", "snps"), P("samples", "snps")),
        out_specs=P("samples", "snps"),
        check_vma=False,
    )
```

```python
import functools
import math

import jax
import jax.numpy as jnp
from jax import lax
from jax.experimental import pallas as pl
from jax.experimental.pallas import tpu as pltpu
from jax.sharding import PartitionSpec as P


def send(value, axis, route):
    count = lax.axis_size(axis)
    pairs = [(source, route(source)) for source in range(count)]
    return lax.ppermute(value, axis, [pair for pair in pairs if pair[1] is not None])


def swap_core(value):
    return send(value, "snps", lambda s: s ^ 1)


def arrival(piece):
    k, half = piece
    return k + 0.5 * half + (1.6 if k % 2 else 0.0)


def strips(samples):
    whole_count = (samples + 2) // 4
    result = []
    for strip in range(4):
        first = strip * (samples + 2) // 4
        begin = first + strip % 2
        wholes = [divmod(begin + n, 2) for n in range(whole_count)]
        cut = divmod(first if strip % 2 else first + whole_count, 2)
        result.append((sorted(wholes, key=arrival), wholes, cut))
    return result


def call_kernel(body, shapes, operands, specs, flops, moved, **more):
    return pl.pallas_call(
        body,
        out_shape=shapes,
        in_specs=specs,
        compiler_params=pltpu.CompilerParams(vmem_limit_bytes=12 * 2**20),
        cost_estimate=pl.CostEstimate(flops=flops, bytes_accessed=moved, transcendentals=0),
        **more,
    )(*operands)


VMEM = pl.BlockSpec(memory_space=pltpu.VMEM)
ANY = pl.BlockSpec(memory_space=pl.ANY)


def encode_body(genotype_ref, mask_ref, first_ref, second_ref, sums_ref,
                dosage_in, mask_in, sems):
    rows = first_ref.shape[0]
    copies = []
    for half in range(2):
        at = pl.ds(half * rows, rows)
        copies.append([
            pltpu.make_async_copy(source.at[at], target.at[at], sems.at[2 * half + n])
            for n, (source, target) in enumerate(((genotype_ref, dosage_in), (mask_ref, mask_in)))
        ])
    for copy in copies[0] + copies[1]:
        copy.start()
    totals = []
    for half, part_ref in enumerate((first_ref, second_ref)):
        for copy in copies[half]:
            copy.wait()
        at = pl.ds(half * rows, rows)
        mask = mask_in[at, :]
        dosage = mask * dosage_in[at, :]
        calls = (dosage + mask).astype(jnp.float32).astype(jnp.bfloat16)
        part_ref[...] = calls
        totals.append([
            jnp.sum(value.astype(jnp.float32), axis=0, keepdims=True) for value in (dosage, mask)
        ])
    for n in range(2):
        sums_ref[n : n + 1, :] = totals[0][n] + totals[1][n]


def encode(genotype, mask):
    rows, columns = genotype.shape
    half = rows // 2
    calls = lambda n: jax.ShapeDtypeStruct((n, columns), jnp.bfloat16)
    return pl.pallas_call(
        encode_body,
        name="encode",
        out_shape=(calls(half), calls(half), jax.ShapeDtypeStruct((2, columns), jnp.float32)),
        in_specs=[ANY, ANY],
        out_specs=(VMEM,) * 3,
        scratch_shapes=[
            pltpu.VMEM((rows, columns), jnp.int32),
            pltpu.VMEM((rows, columns), jnp.int32),
            pltpu.SemaphoreType.DMA((4,)),
        ],
        compiler_params=pltpu.CompilerParams(vmem_limit_bytes=40 * 2**20),
    )(pltpu.with_memory_space_constraint(genotype, pltpu.HBM), pltpu.with_memory_space_constraint(mask, pltpu.HBM))


def factors(sums):
    frequency = (sums[0:1] + 1.0) / (2.0 * sums[1:2] + 2.0)
    return 1.0 + 2.0 * frequency, 1.0 / jnp.sqrt(2.0 * frequency * (1.0 - frequency))


def standardized(calls, shift, scale):
    wide = calls.astype(jnp.float32)
    return jnp.where(wide > 0.0, (wide - shift) * scale, 0.0).astype(jnp.bfloat16)


def left_body(down, first_ref, second_ref, sums_ref, more_ref, left_ref, factors_ref):
    shift, scale = factors(sums_ref[...] + more_ref[...])
    factors_ref[0:1, :] = shift
    factors_ref[1:2, :] = scale
    half = first_ref.shape[0]
    for n, calls_ref in enumerate((first_ref, second_ref)):
        left_ref[pl.ds(n * half, half), :] = standardized(calls_ref[...], shift, scale) * down


def multiply(left, right):
    return lax.dot_general(
        left, right, (((1,), (1,)), ((), ())), preferred_element_type=jnp.float32
    )


def products_body(cases, left_ref, factors_ref, *rest):
    refs, target_refs, right_ref = rest[:-5], rest[-5:-1], rest[-1]
    shift, scale = factors_ref[0:1, :], factors_ref[1:2, :]
    parity = lax.axis_index("samples") % 2
    columns = right_ref.shape[1]

    def work(device, only):
        for n, (strip, at, begin, wanted) in enumerate(cases):
            if wanted == only:
                right_ref[n] = standardized(refs[at][pl.ds(begin, columns), :], shift, scale)
                target_refs[device ^ strip][...] = multiply(left_ref[...], right_ref[n])

    for device in range(len(target_refs)):

        @pl.when(lax.axis_index("snps") == device)
        def _(device=device):
            kinds = {wanted for *_, wanted in cases}
            if None in kinds:
                work(device, None)
            for odd in sorted(kinds - {None}):
                pl.when(parity == odd)(functools.partial(work, device, odd))


def products_more_body(cases, left_ref, factors_ref, *rest):
    products_body(cases, left_ref, factors_ref, *rest[:-9], *rest[-5:])


def add_body(places, at, up, ours_ref, got_ref, other_ref, *rest):
    out_ref, total_ref, sems = rest[-3:]
    height, width = total_ref.shape[0] // 2, total_ref.shape[1]
    device = lax.axis_index("snps")
    for strip, begin in enumerate(places):

        @pl.when(device == strip)
        def _(begin=begin):
            copies = []
            for half in range(2):
                rows = pl.ds(half * height, height)
                other = other_ref[rows, pl.ds(at, width)]
                total_ref[rows, :] = (ours_ref[rows, :] + other + got_ref[rows, :]) * up
                copies.append(pltpu.make_async_copy(
                    total_ref.at[rows], out_ref.at[rows, pl.ds(begin, width)], sems.at[half]
                ))
                copies[half].start()
            for copy in copies:
                copy.wait()


def per_device(genotype, mask):
    samples = lax.axis_size("samples")
    parts = lax.axis_size("snps")
    assert samples % 4 == 0 and samples & (samples - 1) == 0 and parts == 4
    rows, snp_part = genotype.shape
    snp_total = snp_part * parts
    turns = samples // 4
    half_rows = rows // 2
    width = rows * (samples // 2 + 1) // parts

    first, second, sums = encode(genotype, mask)

    along = lambda s: (s - 2) % samples
    even = lax.axis_index("samples") % 2 == 0
    line = [[first, second]]
    for _ in range(1, turns + 1):
        line.append([send(line[-1][h], "samples", along) for h in range(2)])
    side = [None] + [
        [send(line[t][h], "samples", lambda s: s ^ 1) for h in range(2)]
        for t in range(1, turns)
    ]
    side.append([])
    for h in range(2):
        chosen = jnp.where(even, line[turns][h], line[0][1 - h])
        side[turns].append(send(chosen, "samples", lambda s: s ^ 1))

    for bit in range(samples.bit_length() - 1):
        more = send(sums, "samples", lambda s, step=1 << bit: s ^ step)
        if 2 << bit < samples:
            sums = sums + more

    def source(k, h, odd):
        if k == 0:
            return line[0][h], 0
        if k % 2 == 0:
            return line[k // 2][h], 0
        if k == 1 and not odd:
            return side[turns][1 - h], 0
        return side[(k + odd) // 2][h], 0

    table = strips(samples)
    bound = snp_total / 2 * 4 * (samples * rows + 1) / 3
    down = 2.0 ** -math.ceil(math.log2(bound / 32768.0))
    left, pair = call_kernel(
        functools.partial(left_body, down),
        (jax.ShapeDtypeStruct((rows, snp_part), jnp.bfloat16), jax.ShapeDtypeStruct((2, snp_part), jnp.float32)),
        (first, second, sums, more), [VMEM] * 4, 5 * rows * snp_part, 4 * rows * snp_part, out_specs=(VMEM, VMEM),
    )
    count = len(table[0][0])
    quarter = half_rows // 2

    def sources(n):
        result = []
        for strip, (by_arrival, _, cut) in enumerate(table):
            k, h = by_arrival[n] if n < count else cut
            shift_rows = quarter if n == count and strip % 2 else 0
            for odd in range(2):
                array, begin = source(k, h, odd)
                last = (2 * turns - 1 if odd else 1) if k % 2 else (2 * turns if n == 0 else -1)
                result.append((strip, array, begin + shift_rows, odd if k % 2 else None, k == last))
                if k % 2 == 0:
                    break
        return result

    def products(columns, chosen, so_far):
        arrays, cases = [], []
        for strip, array, begin, only, _ in chosen:
            at = next((i for i, known in enumerate(arrays) if known is array), len(arrays))
            if at == len(arrays):
                arrays.append(array)
            cases.append((strip, at, begin, only))
        shape = jax.ShapeDtypeStruct((rows, columns), jnp.float32)
        operands = (left, pair, *arrays, *so_far)
        return call_kernel(
            functools.partial(products_body if not so_far else products_more_body, tuple(cases)),
            (shape,) * 4, operands, [VMEM] * len(operands),
            2 * rows * snp_part * columns * len(chosen), 4 * rows * columns,
            out_specs=(VMEM,) * 4,
            scratch_shapes=[pltpu.VMEM((len(cases), columns, snp_part), jnp.bfloat16)],
            input_output_aliases={len(operands) - 4 + i: i for i in range(len(so_far))},
        )

    pieces, partners = [], []
    for n in range(count + 1):
        columns = half_rows if n < count else quarter
        both = ()
        for wanted in (False, True):
            chosen = [entry for entry in sources(n) if entry[-1] == wanted]
            if chosen:
                both = products(columns, chosen, both)
        own, own_away, neighbour, neighbour_away = both
        other = swap_core(neighbour_away.astype(jnp.float16))
        theirs = (neighbour + other.astype(jnp.float32)).astype(jnp.float16)
        pieces.append((own, send(theirs, "snps", lambda s: s ^ 2)))
        partners.append(own_away.astype(jnp.float16))
    other = swap_core(jnp.concatenate(partners, axis=1)).astype(jnp.float32)
    out = None
    for n, operands in enumerate(pieces):
        places = []
        for strip, (by_arrival, natural, _) in enumerate(table):
            if n < count:
                places.append(natural.index(by_arrival[n]) * half_rows + (strip % 2) * quarter)
            else:
                places.append(0 if strip % 2 else count * half_rows)
        ours, got = operands
        columns = got.shape[1]
        last = () if out is None else (out,)
        operands = (ours, got.astype(jnp.float32), other, *last)
        out = call_kernel(
            functools.partial(add_body, tuple(places), n * half_rows, 1.0 / (down * snp_total)),
            jax.ShapeDtypeStruct((rows, width), jnp.float32), operands,
            [VMEM] * 3 + [ANY] * len(last), rows * columns, 4 * rows * columns,
            out_specs=ANY,
            scratch_shapes=[pltpu.VMEM((rows, columns), jnp.float32), pltpu.SemaphoreType.DMA((2,))],
            input_output_aliases={len(operands) - 1: 0} if last else {},
        )
    return out


def solution(mesh):
    return jax.shard_map(
        per_device,
        mesh=mesh,
        in_specs=(P("samples", "snps"), P("samples", "snps")),
        out_specs=P("samples", "snps"),
        check_vma=False,
    )
```

```python
import functools
import math

import jax
import jax.numpy as jnp
from jax import lax
from jax.experimental import pallas as pl
from jax.experimental.pallas import tpu as pltpu
from jax.sharding import PartitionSpec as P


def send(value, axis, route):
    count = lax.axis_size(axis)
    pairs = [(source, route(source)) for source in range(count)]
    return lax.ppermute(value, axis, [pair for pair in pairs if pair[1] is not None])


def swap_core(value):
    return send(value, "snps", lambda s: s ^ 1)


def arrival(piece):
    k, half = piece
    return k + 0.5 * half + (1.6 if k % 2 else 0.0)


def strips(samples):
    whole_count = (samples + 2) // 4
    result = []
    for strip in range(4):
        first = strip * (samples + 2) // 4
        begin = first + strip % 2
        wholes = [divmod(begin + n, 2) for n in range(whole_count)]
        cut = divmod(first if strip % 2 else first + whole_count, 2)
        result.append((sorted(wholes, key=arrival), wholes, cut))
    return result


def call_kernel(body, shapes, operands, specs, flops, moved, **more):
    return pl.pallas_call(
        body,
        out_shape=shapes,
        in_specs=specs,
        compiler_params=pltpu.CompilerParams(vmem_limit_bytes=12 * 2**20),
        cost_estimate=pl.CostEstimate(flops=flops, bytes_accessed=moved, transcendentals=0),
        **more,
    )(*operands)


VMEM = pl.BlockSpec(memory_space=pltpu.VMEM)
ANY = pl.BlockSpec(memory_space=pl.ANY)


def encode_body(genotype_ref, mask_ref, first_ref, second_ref, sums_ref,
                dosage_in, mask_in, sems):
    rows = first_ref.shape[0]
    copies = []
    for half in range(2):
        at = pl.ds(half * rows, rows)
        copies.append([
            pltpu.make_async_copy(source.at[at], target.at[at], sems.at[2 * half + n])
            for n, (source, target) in enumerate(((genotype_ref, dosage_in), (mask_ref, mask_in)))
        ])
    for copy in copies[0] + copies[1]:
        copy.start()
    totals = []
    for half, part_ref in enumerate((first_ref, second_ref)):
        for copy in copies[half]:
            copy.wait()
        at = pl.ds(half * rows, rows)
        mask = mask_in[at, :]
        dosage = mask * dosage_in[at, :]
        calls = (dosage + mask).astype(jnp.float32).astype(jnp.bfloat16)
        part_ref[...] = calls
        totals.append([
            jnp.sum(value.astype(jnp.float32), axis=0, keepdims=True) for value in (dosage, mask)
        ])
    for n in range(2):
        sums_ref[n : n + 1, :] = totals[0][n] + totals[1][n]


def encode(genotype, mask):
    rows, columns = genotype.shape
    half = rows // 2
    calls = lambda n: jax.ShapeDtypeStruct((n, columns), jnp.bfloat16)
    return pl.pallas_call(
        encode_body,
        name="encode",
        out_shape=(calls(half), calls(half), jax.ShapeDtypeStruct((2, columns), jnp.float32)),
        in_specs=[ANY, ANY],
        out_specs=(VMEM,) * 3,
        scratch_shapes=[
            pltpu.VMEM((rows, columns), jnp.int32),
            pltpu.VMEM((rows, columns), jnp.int32),
            pltpu.SemaphoreType.DMA((4,)),
        ],
        compiler_params=pltpu.CompilerParams(vmem_limit_bytes=40 * 2**20),
    )(pltpu.with_memory_space_constraint(genotype, pltpu.HBM), pltpu.with_memory_space_constraint(mask, pltpu.HBM))


def factors(sums):
    frequency = (sums[0:1] + 1.0) / (2.0 * sums[1:2] + 2.0)
    return 1.0 + 2.0 * frequency, 1.0 / jnp.sqrt(2.0 * frequency * (1.0 - frequency))


def standardized(calls, shift, scale):
    wide = calls.astype(jnp.float32)
    return jnp.where(wide > 0.0, (wide - shift) * scale, 0.0).astype(jnp.bfloat16)


def left_body(down, first_ref, second_ref, sums_ref, more_ref, left_ref, factors_ref):
    shift, scale = factors(sums_ref[...] + more_ref[...])
    factors_ref[0:1, :] = shift
    factors_ref[1:2, :] = scale
    half = first_ref.shape[0]
    for n, calls_ref in enumerate((first_ref, second_ref)):
        left_ref[pl.ds(n * half, half), :] = standardized(calls_ref[...], shift, scale) * down


def multiply(left, right):
    return lax.dot_general(
        left, right, (((1,), (1,)), ((), ())), preferred_element_type=jnp.float32
    )


def products_body(cases, left_ref, factors_ref, *rest):
    refs, target_refs, right_ref = rest[:-5], rest[-5:-1], rest[-1]
    shift, scale = factors_ref[0:1, :], factors_ref[1:2, :]
    parity = lax.axis_index("samples") % 2
    columns = right_ref.shape[1]

    def work(device, only):
        for n, (strip, at, begin, wanted) in enumerate(cases):
            if wanted == only:
                right_ref[n] = standardized(refs[at][pl.ds(begin, columns), :], shift, scale)
                target_refs[device ^ strip][...] = multiply(left_ref[...], right_ref[n])

    for device in range(len(target_refs)):

        @pl.when(lax.axis_index("snps") == device)
        def _(device=device):
            kinds = {wanted for *_, wanted in cases}
            if None in kinds:
                work(device, None)
            for odd in sorted(kinds - {None}):
                pl.when(parity == odd)(functools.partial(work, device, odd))


def products_more_body(cases, left_ref, factors_ref, *rest):
    products_body(cases, left_ref, factors_ref, *rest[:-9], *rest[-5:])


def add_body(places, at, up, ours_ref, got_ref, other_ref, *rest):
    out_ref, total_ref, sem = rest[-3:]
    other = other_ref[:, pl.ds(at, total_ref.shape[1])]
    total_ref[...] = (ours_ref[...] + other + got_ref[...]) * up
    device = lax.axis_index("snps")
    width = total_ref.shape[1]
    for strip, begin in enumerate(places):

        @pl.when(device == strip)
        def _(begin=begin):
            copy = pltpu.make_async_copy(total_ref, out_ref.at[:, pl.ds(begin, width)], sem)
            copy.start()
            copy.wait()


def per_device(genotype, mask):
    samples = lax.axis_size("samples")
    parts = lax.axis_size("snps")
    assert samples % 4 == 0 and samples & (samples - 1) == 0 and parts == 4
    rows, snp_part = genotype.shape
    snp_total = snp_part * parts
    turns = samples // 4
    half_rows = rows // 2
    width = rows * (samples // 2 + 1) // parts

    first, second, sums = encode(genotype, mask)

    along = lambda s: (s - 2) % samples
    even = lax.axis_index("samples") % 2 == 0
    line = [[first, second]]
    for _ in range(1, turns + 1):
        line.append([send(line[-1][h], "samples", along) for h in range(2)])
    side = [None] + [
        [send(line[t][h], "samples", lambda s: s ^ 1) for h in range(2)]
        for t in range(1, turns)
    ]
    side.append([])
    for h in range(2):
        chosen = jnp.where(even, line[turns][h], line[0][1 - h])
        side[turns].append(send(chosen, "samples", lambda s: s ^ 1))

    for bit in range(samples.bit_length() - 1):
        more = send(sums, "samples", lambda s, step=1 << bit: s ^ step)
        if 2 << bit < samples:
            sums = sums + more

    def source(k, h, odd):
        if k == 0:
            return line[0][h], 0
        if k % 2 == 0:
            return line[k // 2][h], 0
        if k == 1 and not odd:
            return side[turns][1 - h], 0
        return side[(k + odd) // 2][h], 0

    table = strips(samples)
    bound = snp_total / 2 * 4 * (samples * rows + 1) / 3
    down = 2.0 ** -math.ceil(math.log2(bound / 32768.0))
    left, pair = call_kernel(
        functools.partial(left_body, down),
        (jax.ShapeDtypeStruct((rows, snp_part), jnp.bfloat16), jax.ShapeDtypeStruct((2, snp_part), jnp.float32)),
        (first, second, sums, more), [VMEM] * 4, 5 * rows * snp_part, 4 * rows * snp_part, out_specs=(VMEM, VMEM),
    )
    count = len(table[0][0])
    quarter = half_rows // 2

    def sources(n):
        result = []
        for strip, (by_arrival, _, cut) in enumerate(table):
            k, h = by_arrival[n] if n < count else cut
            shift_rows = quarter if n == count and strip % 2 else 0
            for odd in range(2):
                array, begin = source(k, h, odd)
                last = (2 * turns - 1 if odd else 1) if k % 2 else (2 * turns if n == 0 else -1)
                result.append((strip, array, begin + shift_rows, odd if k % 2 else None, k == last))
                if k % 2 == 0:
                    break
        return result

    def products(columns, chosen, so_far):
        arrays, cases = [], []
        for strip, array, begin, only, _ in chosen:
            at = next((i for i, known in enumerate(arrays) if known is array), len(arrays))
            if at == len(arrays):
                arrays.append(array)
            cases.append((strip, at, begin, only))
        shape = jax.ShapeDtypeStruct((rows, columns), jnp.float32)
        operands = (left, pair, *arrays, *so_far)
        return call_kernel(
            functools.partial(products_body if not so_far else products_more_body, tuple(cases)),
            (shape,) * 4, operands, [VMEM] * len(operands),
            2 * rows * snp_part * columns * len(chosen), 4 * rows * columns,
            out_specs=(VMEM,) * 4,
            scratch_shapes=[pltpu.VMEM((len(cases), columns, snp_part), jnp.bfloat16)],
            input_output_aliases={len(operands) - 4 + i: i for i in range(len(so_far))},
        )

    pieces, partners = [], []
    for n in range(count + 1):
        columns = half_rows if n < count else quarter
        both = ()
        for wanted in (False, True):
            chosen = [entry for entry in sources(n) if entry[-1] == wanted]
            if chosen:
                both = products(columns, chosen, both)
        own, own_away, neighbour, neighbour_away = both
        other = swap_core(neighbour_away.astype(jnp.float16))
        theirs = (neighbour + other.astype(jnp.float32)).astype(jnp.float16)
        pieces.append((own, send(theirs, "snps", lambda s: s ^ 2)))
        partners.append(own_away.astype(jnp.float16))
    other = swap_core(jnp.concatenate(partners, axis=1)).astype(jnp.float32)
    out = None
    for n, operands in enumerate(pieces):
        places = []
        for strip, (by_arrival, natural, _) in enumerate(table):
            if n < count:
                places.append(natural.index(by_arrival[n]) * half_rows + (strip % 2) * quarter)
            else:
                places.append(0 if strip % 2 else count * half_rows)
        ours, got = operands
        columns = got.shape[1]
        last = () if out is None else (out,)
        operands = (ours, got.astype(jnp.float32), other, *last)
        out = call_kernel(
            functools.partial(add_body, tuple(places), n * half_rows, 1.0 / (down * snp_total)),
            jax.ShapeDtypeStruct((rows, width), jnp.float32), operands,
            [VMEM] * 3 + [ANY] * len(last), rows * columns, 4 * rows * columns,
            out_specs=ANY,
            scratch_shapes=[pltpu.VMEM((rows, columns), jnp.float32), pltpu.SemaphoreType.DMA],
            input_output_aliases={len(operands) - 1: 0} if last else {},
        )
    return out


def solution(mesh):
    return jax.shard_map(
        per_device,
        mesh=mesh,
        in_specs=(P("samples", "snps"), P("samples", "snps")),
        out_specs=P("samples", "snps"),
        check_vma=False,
    )
```
